256 devices in a mesh: cond: 2 (over z_hi), gx: 8 (over y, core), yz: 16 (over x, z_lo).
Axes of the slice: x: 4, y: 4, z: 8 (z_hi: 2, z_lo: 4; z = z_hi * 4 + z_lo), core: 2. Of those that a mesh axis runs over, the one named last changes fastest.
Arguments:
- adjoint: float32 [2, 5, 64, 256, 256], P('cond', None, 'gx', 'yz'), may hold values from -6 to 6
- objective_gradient: float32 [2, 5, 64, 256, 256], P('cond', None, 'gx', 'yz'), may hold values from -6 to 6
- diagonal: float32 [64, 256, 256], P('gx', 'yz'), may hold values from 4 to 12
- flux_blocks: float32 [2, 6, 5, 5], P('cond'), may hold values from -1 to 1
- flux_sensitivity: bfloat16 [2, 5, 64, 256, 256], P('cond', None, 'gx', 'yz'), may hold values from -6 to 6
- surface_mask: int32 [64, 256, 256], P('gx', 'yz'), may hold values 0 or 1
- patch_band_slot: int32 [64, 256], P('gx', 'yz'), may hold values from 0 to 62
- design_basis: float32 [256, 128], replicated, may hold values from -0.015625 to 0.015625
- condition_weights: int32 [2], replicated, may hold values from 1 to 999, as said below
Outputs:
- smoothed: float32 [2, 5, 64, 256, 256], P('cond', None, 'gx', 'yz')
- residual: float32 [2, 5, 64, 256, 256], P('cond', None, 'gx', 'yz')
- design_gradient: float32 [4096], P(('gx', 'yz'))
The draws below stay inside these ranges and needn't reach their ends.
Inputs may be any that keep to these rules, and one draw needn't show every extreme that they name: `condition_weights`: positive integer weights; one condition has weight 999.
All inputs are finite; a program needn't handle non-finite values. No bound on the sum of `surface_mask` on one device may be relied on, other than what follows from the above.
Results may differ from the reference program's by a relative error of at most 0.0003.
Values sent between devices are 32-bit elements; how exact they have to be, the bound alone decides.
A program may use at most 64 MiB of HBM per device.

```python
import math
import jax
import jax.numpy as jnp
import numpy as np
from jax import lax

NZ = 256
NVAR = 5
BAND = 128
BAND_SLOTS = 63
COND = 2
CELLS_FIRST = 64
CELLS_SECOND = 256


def draw_condition_weights(key, part):
    drawn = jax.random.randint(jax.random.fold_in(key, 7), (COND,), 1, 1000, dtype=jnp.int32)
    chosen = jax.random.randint(jax.random.fold_in(key, 8), (), 0, COND, dtype=jnp.int32)
    return jnp.where(jnp.arange(COND, dtype=jnp.int32) == chosen, jnp.int32(999), drawn)


def touch_ends(array, own_key, least, top_value):
    longest = array.shape.index(max(array.shape))
    spots = []
    for shift in (0, 1):
        where = [jax.random.randint(jax.random.fold_in(own_key, axis), (), 0, length) for axis, length in enumerate(array.shape)]
        where[longest] = (where[longest] + shift) % array.shape[longest]
        spots.append(tuple(where))
    return array.at[spots[0]].set(least).at[spots[1]].set(top_value)


def level_of(stream_key, dims, cuts, low, high):
    level = 1.0
    for dim, blocks in cuts:
        steps = jax.random.uniform(jax.random.fold_in(jax.random.fold_in(stream_key, 6), dim), (blocks,), jnp.float32, low / len(cuts), high / len(cuts))
        level = level * jnp.repeat(jnp.exp(steps), dims[dim] // blocks).reshape((-1,) + (1,) * (len(dims) - 1 - dim))
    return level


def rank_table(count, skew):
    loads = [(1 << 20) // math.isqrt(grade ** skew) + 1 for grade in range(1, count + 1)]
    scale = 1 + sum(loads) // (1 << 30)
    return np.cumsum(np.array([max(1, weight // scale) for weight in loads]))


def ranked(own_key, extent, amount, lean):
    grid = rank_table(amount, lean)
    lot = jax.random.randint(jax.random.fold_in(own_key, 1), extent, 0, int(grid[amount - 1]))
    grade = jnp.searchsorted(jnp.asarray(grid, jnp.int32), lot, side="right")
    return jax.random.permutation(jax.random.fold_in(own_key, 2), amount)[grade].astype(jnp.int32)


def centred(key, shape, width, limit, pieces=(), kind=jnp.bfloat16):
    values = width * jax.random.normal(key, shape, jnp.float32)
    if pieces:
        values = values * level_of(key, shape, pieces, -0.22, 0.18)
    return jnp.clip(values, -limit, limit).astype(kind)


def setup_inputs(seed: int = 0) -> dict:
    streams_of = jax.random.split(jax.random.key(seed), 10)
    return {
        "adjoint": centred(streams_of[0], (COND, NVAR, CELLS_FIRST, CELLS_SECOND, NZ), 1.0, 6.0, ((0, 2), (2, 8), (3, 16)), jnp.float32),
        "objective_gradient": centred(streams_of[1], (COND, NVAR, CELLS_FIRST, CELLS_SECOND, NZ), 1.0, 6.0, ((0, 2), (2, 8), (3, 16)), jnp.float32),
        "diagonal": jnp.clip(jnp.exp(math.log(12.0) - 1.0986123 * jax.random.uniform(streams_of[2], (CELLS_FIRST, CELLS_SECOND, NZ), jnp.float32) ** level_of(streams_of[2], (CELLS_FIRST, CELLS_SECOND, NZ), ((0, 8), (1, 16)), -0.2, 0.2)), 4.0, 12.0),
        "flux_blocks": centred(streams_of[3], (COND, 6, NVAR, NVAR), (6 * NVAR) ** -0.5, 1.0, ((0, 2),), jnp.float32),
        "flux_sensitivity": centred(streams_of[4], (COND, NVAR, CELLS_FIRST, CELLS_SECOND, NZ), 1.0, 6.0, ((0, 2), (2, 8), (3, 16))),
        "surface_mask": touch_ends((jax.random.randint(streams_of[5], (CELLS_FIRST, CELLS_SECOND, NZ), 0, 4) < 1).astype(jnp.int32), jax.random.fold_in(streams_of[5], 1), 0, 1),
        "patch_band_slot": touch_ends(ranked(streams_of[6], (CELLS_FIRST, CELLS_SECOND), BAND_SLOTS, 2), jax.random.fold_in(streams_of[6], 3), 0, BAND_SLOTS - 1).astype(jnp.int32),
        "design_basis": centred(streams_of[7], (NZ, BAND), (NZ * CELLS_FIRST * CELLS_SECOND // 32) ** -0.5, 0.015625, (), jnp.float32),
        "condition_weights": draw_condition_weights(jax.random.fold_in(streams_of[9], 71), 0),
    }


relaxation = 0.8
neighbour_starts = ((2, 1, 1), (0, 1, 1), (1, 2, 1), (1, 0, 1), (1, 1, 2), (1, 1, 0))


def apply_operator(padded_field, diagonal, blocks):
    size_x = padded_field.shape[1] - 2
    size_y = padded_field.shape[2] - 2
    size_z = padded_field.shape[3] - 2
    result = diagonal * padded_field[:, 1:-1, 1:-1, 1:-1]
    for direction in range(6):
        start_x, start_y, start_z = neighbour_starts[direction]
        shifted = padded_field[:, start_x:start_x + size_x, start_y:start_y + size_y, start_z:start_z + size_z]
        result = result - jnp.einsum("ec,exyz->cxyz", blocks[direction], shifted, precision=lax.Precision.HIGHEST)
    return result


def spread_bands(slot_lookup):
    halfway = slot_lookup.shape[1] // 2
    first_half = jnp.pad(slot_lookup[:, :halfway], ((0, 1), (0, 0)))
    second_half = jnp.pad(slot_lookup[:, halfway:], ((1, 0), (0, 0)))
    return (first_half + second_half).reshape(-1)


def reference(adjoint, objective_gradient, diagonal, flux_blocks, flux_sensitivity, surface_mask, patch_band_slot, design_basis, condition_weights):
    def condition_solve(inputs):
        start_field, source, blocks, sensitivity = inputs

        def operate(values):
            return apply_operator(jnp.pad(values, ((0, 0), (1, 1), (1, 1), (1, 1))), diagonal, blocks)

        relaxed = start_field + (relaxation * (source - operate(start_field))) / diagonal
        smoothed = relaxed + (relaxation * (source - operate(relaxed))) / diagonal
        residual = source - operate(smoothed)
        surface = surface_mask.astype(jnp.float32) * jnp.sum(smoothed * sensitivity.astype(jnp.float32), axis=0)
        projected_gradient = jnp.dot(surface.reshape(-1, NZ), design_basis, precision=lax.Precision.HIGHEST, preferred_element_type=jnp.float32)
        slot_lookup = jax.ops.segment_sum(projected_gradient, patch_band_slot.reshape(-1), num_segments=BAND_SLOTS)
        return smoothed, residual, spread_bands(slot_lookup)

    smoothed, residual, gradients = lax.map(condition_solve, (adjoint, objective_gradient, flux_blocks, flux_sensitivity))
    weights_float = condition_weights.astype(jnp.float32)
    shares = weights_float / jnp.sum(weights_float)
    design_gradient = jnp.sum(shares[:, None] * gradients, axis=0)
    return smoothed, residual, design_gradient
```

```python
import functools

import jax
import jax.numpy as jnp
from jax import lax
from jax.experimental import pallas as pl
from jax.experimental.pallas import tpu as pltpu
from jax.sharding import Mesh
from jax.sharding import PartitionSpec as P

NDES = 4096
NVAR = 5
LANES = 128
SUBLANES = 8
AXES = ("cond", "gx_0", "gx_1", "yz_0", "yz_1")
GX = ("gx_0", "gx_1")
YZ = ("yz_0", "yz_1")
GX_YZ = GX + YZ
MESH = pl.DeviceIdType.MESH
RELAX = 0.8
X_HI, X_LO, Y_HI, Y_LO, Z_HI, Z_LO = range(6)


def kernel(
    dims,
    adjoint,
    objective,
    diagonal,
    sensitivity,
    mask,
    basis,
    blocks,
    weights,
    slots,
    smoothed,
    residual,
    gradient,
    start,
    relaxed,
    source,
    diag,
    ratio,
    sens,
    surface_mask,
    base,
    surface,
    onehot,
    halo_x,
    halo_y,
    face_y,
    outgoing,
    plane_in,
    row_out,
    column_in,
    local_sem,
    halo_send,
    halo_recv,
    plane_send,
    plane_recv,
    column_send,
    column_recv,
):
    n_cond, n_y, n_core, n_x, n_zl = dims
    nx, ny = slots.shape
    rows = nx * ny
    n_row, n_col = ny // SUBLANES, basis.shape[0] // LANES
    span = n_row * n_col * SUBLANES
    n_gx, n_yz, n_plane, n_z = n_y * n_core, n_x * n_zl, n_y * n_core * n_x, n_cond * n_zl

    cond, y, core, x, zl = (lax.axis_index(a) for a in AXES)
    gx, yz = y * n_core + core, x * n_zl + zl
    plane, z = gx * n_x + x, cond * n_zl + zl

    def at_gx(g):
        return (cond, g // n_core, g % n_core, x, zl)

    def at_yz(q):
        return (cond, y, core, q // n_zl, q % n_zl)

    def at_plane(p):
        g = p // n_x
        return (cond, g // n_core, g % n_core, p % n_x, zl)

    def at_z(q):
        return (q // n_zl, y, core, x, q % n_zl)

    pairs = (
        (adjoint, start),
        (diagonal, diag),
        (objective, source),
        (mask, surface_mask),
        (sensitivity, sens),
        (basis, base),
    )
    loads = [pltpu.make_async_copy(a, b, local_sem.at[i]) for i, (a, b) in enumerate(pairs)]
    load_start, load_diag, load_source, load_mask, load_sens, load_base = loads
    for load in loads:
        load.start()

    barrier = pltpu.get_barrier_semaphore()

    def greet(target):
        pl.semaphore_signal(barrier, inc=1, device_id=target, device_id_type=MESH)

    step_up = jnp.logical_and(zl == n_zl - 1, x < n_x - 1)
    step_down = jnp.logical_and(zl == 0, x > 0)

    @pl.when(step_up)
    def _():
        greet(at_yz(yz + 1))

    @pl.when(step_down)
    def _():
        greet(at_yz(yz - 1))

    for o in range(1, n_z):
        greet(at_z((z + o) % n_z))
    for o in range(1, n_plane):
        greet(at_plane((plane + o) % n_plane))

    sides = (
        (gx > 0, gx < n_gx - 1),
        (yz > 0, yz < n_yz - 1),
    )

    for axis, buffer in ((0, halo_x), (1, halo_y)):
        for side in range(2):

            @pl.when(jnp.logical_not(sides[axis][side]))
            def _(buffer=buffer, side=side):
                buffer[:, side] = jnp.zeros_like(buffer[:, side])

    def halo_copy(field, turn, axis, side):
        index = 2 * axis + side
        if axis == 0:
            src = field.at[:, pl.ds((nx - 1) * span if side else 0, span)]
            dst = halo_x.at[turn, 1 - side]
            target = at_gx(gx + 1 if side else gx - 1)
        else:
            src = face_y.at[turn, side]
            dst = halo_y.at[turn, 1 - side]
            target = at_yz(yz + 1 if side else yz - 1)
        return pltpu.make_async_remote_copy(
            src_ref=src,
            dst_ref=dst,
            send_sem=halo_send.at[turn, index],
            recv_sem=halo_recv.at[turn, 2 * axis + 1 - side],
            device_id=target,
            device_id_type=MESH,
        )

    def each_side(body):
        for axis in (1, 0):
            for side in range(2):

                @pl.when(sides[axis][side])
                def _(axis=axis, side=side):
                    body(axis, side)

    def line(side, c):
        first = ((n_row - 1) * n_col + c) * SUBLANES + SUBLANES - 1 if side else c * SUBLANES
        return pl.ds(first, nx, stride=span)

    def pack_faces(field, turn):
        for side in range(2):
            for e in range(NVAR):
                for c in range(n_col):
                    face_y[turn, side, e, pl.ds(c * nx, nx), :] = field[e, line(side, c), :]

    def send_faces(field, turn):
        each_side(lambda axis, side: halo_copy(field, turn, axis, side).start())

    def wait_faces(turn):
        def body(axis, side):
            pltpu.make_async_remote_copy(
                src_ref=(halo_x if axis == 0 else halo_y).at[turn, side],
                dst_ref=(halo_x if axis == 0 else halo_y).at[turn, side],
                send_sem=halo_send.at[turn, 2 * axis + side],
                recv_sem=halo_recv.at[turn, 2 * axis + side],
                device_id=at_gx(gx) if axis == 0 else at_yz(yz),
                device_id_type=MESH,
            ).wait_recv()

        each_side(body)

    def drain_faces(field, turn):
        each_side(lambda axis, side: halo_copy(field, turn, axis, side).wait_send())

    tiles = [(r, c) for r in range(n_row) for c in range(n_col)]

    def window(block, r, c):
        at = block * span + (r * n_col + c) * SUBLANES
        return pl.ds(at if isinstance(at, int) else pl.multiple_of(at, SUBLANES), SUBLANES)

    def neighbours(field, block, lo, hi):
        sub = lax.broadcasted_iota(jnp.int32, (SUBLANES, LANES), 0)
        lane = lax.broadcasted_iota(jnp.int32, (SUBLANES, LANES), 1)
        zero = jnp.zeros((SUBLANES, LANES), jnp.float32)

        def tile_of(e, b, r, c):
            return field[e, window(b, r, c), :]

        total = [[None] * len(tiles) for _ in range(NVAR)]
        for e in range(NVAR):
            here = {rc: tile_of(e, block, *rc) for rc in tiles}
            terms = {}
            if hi:
                terms[X_HI] = {rc: tile_of(e, block + 1, *rc) for rc in tiles}
            if lo:
                terms[X_LO] = {rc: tile_of(e, block - 1, *rc) for rc in tiles}
            for d, shift, axis, index, edge in (
                (Y_HI, SUBLANES - 1, 0, sub, SUBLANES - 1),
                (Y_LO, 1, 0, sub, 0),
                (Z_HI, LANES - 1, 1, lane, LANES - 1),
                (Z_LO, 1, 1, lane, 0),
            ):
                turned = {rc: pltpu.roll(here[rc], shift, axis) for rc in tiles}
                step = 1 if edge else -1
                moved = {}
                for r, c in tiles:
                    beside = (r + step, c) if axis == 0 else (r, c + step)
                    moved[r, c] = jnp.where(index == edge, turned.get(beside, zero), turned[r, c])
                terms[d] = moved
            for d, values in terms.items():
                for k in range(NVAR):
                    coef = blocks[0, d, e, k]
                    for i, rc in enumerate(tiles):
                        part = coef * values[rc]
                        total[k][i] = part if total[k][i] is None else total[k][i] + part
        return total

    def over_blocks(body):
        body(0, False, True)

        def inner(b, carry):
            body(b, True, True)
            return carry

        lax.fori_loop(1, nx - 1, inner, 0)
        body(nx - 1, True, False)

    def sweep(field, result):
        def body(block, lo, hi):
            total = neighbours(field, block, lo, hi)
            for i, rc in enumerate(tiles):
                at = window(block, *rc)
                scale = ratio[at, :]
                for k in range(NVAR):
                    result[k, at, :] = (1.0 - RELAX) * field[k, at, :] + scale * (
                        source[k, at, :] + total[k][i]
                    )

        over_blocks(body)

    def operate(field, result):
        def body(block, lo, hi):
            total = neighbours(field, block, lo, hi)
            for i, rc in enumerate(tiles):
                at = window(block, *rc)
                scale = diag[at, :]
                for k in range(NVAR):
                    result[k, at, :] = source[k, at, :] - scale * field[k, at, :] + total[k][i]

        over_blocks(body)

    def add_halos(turn, result, scale):
        for axis, buffer in ((0, halo_x), (1, halo_y)):
            for side in range(2):
                d = (X_LO, X_HI, Y_LO, Y_HI)[2 * axis + side]
                if axis == 0:
                    first = (nx - 1) * span if side else 0
                    parts = [(pl.ds(first + i, SUBLANES), pl.ds(i, SUBLANES)) for i in range(0, span, SUBLANES)]
                else:
                    parts = [(line(side, c), pl.ds(c * nx, nx)) for c in range(n_col)]
                for at, place in parts:
                    factor = None if scale is None else scale[at, :]
                    outside = [buffer[turn, side, e, place, :] for e in range(NVAR)]
                    for k in range(NVAR):
                        part = blocks[0, d, 0, k] * outside[0]
                        for e in range(1, NVAR):
                            part = part + blocks[0, d, e, k] * outside[e]
                        part = part if factor is None else factor * part
                        result[k, at, :] = result[k, at, :] + part

    load_start.wait()
    pack_faces(start, 0)
    pl.semaphore_wait(
        barrier, n_z + n_plane - 2 + step_up.astype(jnp.int32) + step_down.astype(jnp.int32)
    )
    send_faces(start, 0)

    load_diag.wait()
    ratio[...] = RELAX / diag[...]
    load_source.wait()
    sweep(start, relaxed)

    pick = lax.broadcasted_iota(jnp.int32, (ny, rows), 1) % ny == lax.broadcasted_iota(jnp.int32, (ny, rows), 0)
    spread = jnp.dot(
        slots[...].astype(jnp.float32), pick.astype(jnp.float32), preferred_element_type=jnp.float32
    )
    own = lax.broadcasted_iota(jnp.int32, (nx, rows), 1) // ny == lax.broadcasted_iota(jnp.int32, (nx, rows), 0)
    slot_row = jnp.sum(jnp.where(own, spread, 0.0), axis=0, keepdims=True)
    n_out = NDES // LANES
    number = lax.broadcasted_iota(jnp.int32, (3 * n_out, rows), 0)
    third = number // n_out
    wanted = 2 * (number % n_out) + jnp.where(third == 0, 0, jnp.where(third == 1, -1, 1))
    onehot[...] = jnp.where(slot_row == wanted.astype(jnp.float32), 1.0, 0.0)

    wait_faces(0)
    add_halos(0, relaxed, ratio)
    pack_faces(relaxed, 1)
    send_faces(relaxed, 1)
    sweep(relaxed, smoothed)
    load_mask.wait()
    load_sens.wait()
    load_base.wait()
    drain_faces(start, 0)

    wait_faces(1)
    add_halos(1, smoothed, ratio)
    pack_faces(smoothed, 2)
    send_faces(smoothed, 2)

    for block in range(nx):
        for c in range(n_col):
            cols = pl.ds(c * LANES, LANES)
            weight = [sens[k, pl.ds(block * ny, ny), cols].astype(jnp.float32) for k in range(NVAR)]
            for r in range(n_row):
                at = window(block, r, c)
                part = [
                    smoothed[k, at, :] * weight[k][r * SUBLANES : (r + 1) * SUBLANES] for k in range(NVAR)
                ]
                surface[pl.ds(block * ny + r * SUBLANES, SUBLANES), cols] = surface_mask[at, :].astype(
                    jnp.float32
                ) * functools.reduce(jnp.add, part)
    projected = jnp.dot(
        surface[...], base[...], precision=lax.Precision.HIGHEST, preferred_element_type=jnp.float32
    )
    looked = jnp.dot(
        onehot[...], projected, precision=lax.Precision.HIGHEST, preferred_element_type=jnp.float32
    )
    even, before, after = (looked[i * n_out : (i + 1) * n_out] for i in range(3))
    half = lax.broadcasted_iota(jnp.int32, (n_out, LANES), 1) < LANES // 2
    swapped = pltpu.roll(jnp.where(half, after, before), LANES // 2, 1)
    whole = jnp.full((n_out, LANES), (weights[0] + weights[1]).astype(jnp.float32))
    mine = jnp.where(cond == 0, weights[0], weights[1]).astype(jnp.float32)
    scaled = (even + swapped) * (jnp.full((n_out, LANES), mine) / whole)
    outgoing[...] = scaled.reshape(n_out, 1, LANES)

    def plane_copy(o):
        target = (plane + o) % n_plane
        return pltpu.make_async_remote_copy(
            src_ref=outgoing.at[target],
            dst_ref=plane_in.at[plane],
            send_sem=plane_send,
            recv_sem=plane_recv,
            device_id=at_plane(target),
            device_id_type=MESH,
        )

    for o in range(1, n_plane):
        plane_copy(o).start()
    plane_in[plane] = outgoing[plane]

    operate(smoothed, residual)
    drain_faces(relaxed, 1)

    everyone = pltpu.make_async_remote_copy(
        src_ref=outgoing.at[pl.ds(0, n_plane - 1)],
        dst_ref=plane_in.at[pl.ds(0, n_plane - 1)],
        send_sem=plane_send,
        recv_sem=plane_recv,
        device_id=at_plane(plane),
        device_id_type=MESH,
    )
    everyone.wait_recv()
    row = plane_in[0]
    for i in range(1, n_plane):
        row = row + plane_in[i]
    row_out[0] = row
    column_in[z] = row

    def column_copy(o):
        return pltpu.make_async_remote_copy(
            src_ref=row_out.at[0],
            dst_ref=column_in.at[z],
            send_sem=column_send.at[o - 1],
            recv_sem=column_recv,
            device_id=at_z((z + o) % n_z),
            device_id_type=MESH,
        )

    for o in range(1, n_z):
        column_copy(o).start()

    wait_faces(2)
    add_halos(2, residual, None)
    everyone.wait_send()
    drain_faces(smoothed, 2)

    pltpu.make_async_remote_copy(
        src_ref=column_in.at[pl.ds(0, n_z - 1)],
        dst_ref=column_in.at[pl.ds(0, n_z - 1)],
        send_sem=column_send.at[0],
        recv_sem=column_recv,
        device_id=at_z(z),
        device_id_type=MESH,
    ).wait_recv()
    row = column_in[0]
    for i in range(1, n_z):
        row = row + column_in[i]
    width = LANES // n_zl
    part = row[:, :width]
    for q in range(1, n_zl):
        part = jnp.where(zl == q, row[:, q * width : (q + 1) * width], part)
    gradient[...] = part
    for o in range(1, n_z):
        column_copy(o).wait_send()


def to_tiles(array):
    *lead, ny, nz = array.shape
    split = array.reshape(*lead, ny // SUBLANES, SUBLANES, nz // LANES, LANES)
    return jnp.swapaxes(split, -2, -3).reshape(*lead[:-1], -1, LANES)


def from_tiles(array, shape):
    *lead, ny, nz = shape
    split = array.reshape(*lead, ny // SUBLANES, nz // LANES, SUBLANES, LANES)
    return jnp.swapaxes(split, -2, -3).reshape(shape)


def local(
    dims,
    adjoint,
    objective_gradient,
    diagonal,
    flux_blocks,
    flux_sensitivity,
    surface_mask,
    patch_band_slot,
    design_basis,
    condition_weights,
):
    _, nvar, nx, ny, nz = adjoint.shape
    rows = nx * ny
    n_cond, n_y, n_core, n_x, n_zl = dims
    n_plane, n_z = n_y * n_core * n_x, n_cond * n_zl
    f32 = jnp.float32
    flat = nx * ny * nz // LANES
    field, cell = (nvar, flat, LANES), (flat, LANES)
    anywhere = pl.BlockSpec(memory_space=pl.ANY)
    scalars = pl.BlockSpec(memory_space=pltpu.SMEM)
    vmem = pl.BlockSpec(memory_space=pltpu.VMEM)
    dma = pltpu.SemaphoreType.DMA
    smoothed, residual, gradient = pl.pallas_call(
        functools.partial(kernel, dims),
        out_shape=(
            jax.ShapeDtypeStruct(field, f32),
            jax.ShapeDtypeStruct(field, f32),
            jax.ShapeDtypeStruct((1, LANES // n_zl), f32),
        ),
        in_specs=[anywhere] * 6 + [scalars] * 2 + [vmem],
        out_specs=(vmem, vmem, vmem),
        scratch_shapes=[
            pltpu.VMEM(field, f32),
            pltpu.VMEM(field, f32),
            pltpu.VMEM(field, f32),
            pltpu.VMEM(cell, f32),
            pltpu.VMEM(cell, f32),
            pltpu.VMEM((nvar, rows, nz), jnp.bfloat16),
            pltpu.VMEM(cell, jnp.int32),
            pltpu.VMEM(design_basis.shape, f32),
            pltpu.VMEM((rows, nz), f32),
            pltpu.VMEM((3 * NDES // LANES, rows), f32),
            pltpu.VMEM((3, 2, nvar, ny * nz // LANES, LANES), f32),
            pltpu.VMEM((3, 2, nvar, nx * nz // LANES, LANES), f32),
            pltpu.VMEM((3, 2, nvar, nx * nz // LANES, LANES), f32),
            pltpu.VMEM((NDES // LANES, 1, LANES), f32),
            pltpu.VMEM((n_plane, 1, LANES), f32),
            pltpu.VMEM((1, 1, LANES), f32),
            pltpu.VMEM((n_z, 1, LANES), f32),
            dma((6,)),
            dma((3, 4)),
            dma((3, 4)),
            dma,
            dma,
            dma((n_z - 1,)),
            dma,
        ],
        compiler_params=pltpu.CompilerParams(
            collective_id=0, has_side_effects=True, vmem_limit_bytes=40 * 1024 * 1024
        ),
        name="adjoint_step",
    )(
        to_tiles(adjoint[0]),
        to_tiles(objective_gradient[0]),
        to_tiles(diagonal),
        flux_sensitivity.reshape(nvar, rows, nz),
        to_tiles(surface_mask),
        design_basis,
        flux_blocks,
        condition_weights,
        patch_band_slot,
    )
    whole = (1, nvar, nx, ny, nz)
    return from_tiles(smoothed, whole), from_tiles(residual, whole), gradient.reshape(-1)


def solution(mesh):
    dims = (mesh.shape["cond"], 4, 2, 4, 4)
    torus = Mesh(mesh.devices.reshape(dims), AXES)
    in_specs = (
        P("cond", None, GX, YZ, None),
        P("cond", None, GX, YZ, None),
        P(GX, YZ, None),
        P("cond", None, None, None),
        P("cond", None, GX, YZ, None),
        P(GX, YZ, None),
        P(GX, YZ),
        P(),
        P(),
    )
    out_specs = (P("cond", None, GX, YZ, None), P("cond", None, GX, YZ, None), P(GX_YZ))
    return jax.shard_map(
        functools.partial(local, dims), mesh=torus, in_specs=in_specs, out_specs=out_specs, check_vma=False
    )
```

```python
import functools

import jax
import jax.numpy as jnp
from jax import lax
from jax.experimental import pallas as pl
from jax.experimental.pallas import tpu as pltpu
from jax.sharding import Mesh
from jax.sharding import PartitionSpec as P

NDES = 4096
NVAR = 5
LANES = 128
SUBLANES = 8
AXES = ("cond", "gx_0", "gx_1", "yz_0", "yz_1")
GX = ("gx_0", "gx_1")
YZ = ("yz_0", "yz_1")
GX_YZ = GX + YZ
MESH = pl.DeviceIdType.MESH
RELAX = 0.8
KERNEL_VMEM = 40 * 1024 * 1024
X_HI, X_LO, Y_HI, Y_LO, Z_HI, Z_LO = range(6)


def kernel(
    dims,
    adjoint,
    objective,
    diagonal,
    sensitivity,
    mask,
    basis,
    blocks_in,
    weights_in,
    slots_in,
    smoothed,
    residual,
    gradient,
    blocks,
    weights,
    slots,
    start,
    relaxed,
    source,
    diag,
    ratio,
    sens,
    surface_mask,
    base,
    surface,
    onehot,
    mass,
    halo_x,
    halo_y,
    face_x,
    face_y,
    slots_beside,
    outgoing,
    plane_in,
    row_out,
    column_in,
    local_sem,
    halo_send,
    halo_recv,
    slots_send,
    slots_recv,
    gate,
    plane_send,
    plane_recv,
    column_send,
    column_recv,
):
    n_cond, n_y, n_core, n_x, n_zl = dims
    nx, ny = slots.shape
    rows = nx * ny
    n_row, n_col = ny // SUBLANES, basis.shape[0] // LANES
    span = n_row * n_col * SUBLANES
    n_gx, n_yz, n_plane, n_z = n_y * n_core, n_x * n_zl, n_y * n_core * n_x, n_cond * n_zl

    cond, y, core, x, zl = (lax.axis_index(a) for a in AXES)
    gx, yz = y * n_core + core, x * n_zl + zl
    plane, z = gx * n_x + x, cond * n_zl + zl

    def at_gx(g):
        return (cond, lax.div(g, n_core), lax.rem(g, n_core), x, zl)

    def at_yz(q):
        return (cond, y, core, lax.div(q, n_zl), lax.rem(q, n_zl))

    def around(index, size):
        return [index] + [lax.rem(index + o, size) for o in range(1, size)]

    conds, ys, cores, xs, zls = (around(i, n) for i, n in zip((cond, y, core, x, zl), dims))
    plane_targets = [
        ((cond, b, c, d, zl), (b * n_core + c) * n_x + d)
        for i, b in enumerate(ys)
        for j, c in enumerate(cores)
        for k, d in enumerate(xs)
        if i or j or k
    ]
    z_targets = [(a, y, core, x, e) for i, a in enumerate(conds) for j, e in enumerate(zls) if i or j]

    pairs = (
        (adjoint, start),
        (diagonal, diag),
        (objective, source),
        (mask, surface_mask),
        (sensitivity, sens),
        (basis, base),
        (blocks_in, blocks),
        (weights_in, weights),
        (slots_in, slots),
    )
    loads = [pltpu.make_async_copy(a, b, local_sem.at[i]) for i, (a, b) in enumerate(pairs)]
    load_start, load_diag, load_source, load_mask, load_sens, load_base = loads[:6]
    for load in loads:
        load.start()

    barrier = pltpu.get_barrier_semaphore()

    def greet(target):
        pl.semaphore_signal(barrier, inc=1, device_id=target, device_id_type=MESH)

    step_up = jnp.logical_and(zl == n_zl - 1, x < n_x - 1)
    step_down = jnp.logical_and(zl == 0, x > 0)

    @pl.when(step_up)
    def _():
        greet(at_yz(yz + 1))

    @pl.when(step_down)
    def _():
        greet(at_yz(yz - 1))

    line_gx = [(cond, b, c, x, zl) for i, b in enumerate(ys) for j, c in enumerate(cores) if i or j]
    mirror = (n_cond - 1 - cond, y, core, x, n_zl - 1 - zl)
    greeted = (
        line_gx + [(cond, y, core, d, zl) for d in xs[1:]] + [(cond, y, core, x, e) for e in zls[1:]] + [mirror]
    )
    for target in greeted:
        greet(target)

    sides = (
        (gx > 0, gx < n_gx - 1),
        (yz > 0, yz < n_yz - 1),
    )

    for axis, buffer in ((0, halo_x), (1, halo_y)):
        for side in range(2):

            @pl.when(jnp.logical_not(sides[axis][side]))
            def _(buffer=buffer, side=side, index=2 * axis + side):
                buffer[:, side] = jnp.zeros_like(buffer[:, side])
                slots_beside[index] = jnp.zeros_like(slots_beside[index])

    def halo_copy(field, turn, axis, side):
        index = 2 * axis + side
        if axis == 0:
            if field is None:
                src = face_x.at[side]
            else:
                src = field.at[:, pl.ds((nx - 1) * span if side else 0, span)]
            dst = halo_x.at[turn, 1 - side]
            target = at_gx(gx + 1 if side else gx - 1)
        else:
            src = face_y.at[turn, side]
            dst = halo_y.at[turn, 1 - side]
            target = at_yz(yz + 1 if side else yz - 1)
        return pltpu.make_async_remote_copy(
            src_ref=src,
            dst_ref=dst,
            send_sem=halo_send.at[turn, index],
            recv_sem=halo_recv.at[turn, 2 * axis + 1 - side],
            device_id=target,
            device_id_type=MESH,
        )

    def each_side(body):
        for axis in (1, 0):
            for side in range(2):

                @pl.when(sides[axis][side])
                def _(axis=axis, side=side):
                    body(axis, side)

    def line(side, c):
        first = ((n_row - 1) * n_col + c) * SUBLANES + SUBLANES - 1 if side else c * SUBLANES
        return pl.ds(first, nx, stride=span)

    def pack_faces(field, turn):
        for side in range(2):
            for e in range(NVAR):
                for c in range(n_col):
                    face_y[turn, side, e, pl.ds(c * nx, nx), :] = field[e, line(side, c), :]

    far = (zl == 0, zl == n_zl - 1)

    def send_faces(field, turn):
        for side in range(2):

            @pl.when(jnp.logical_and(sides[1][side], far[side]))
            def _(side=side):
                halo_copy(field, turn, 1, side).start()

        for side in range(2):

            @pl.when(jnp.logical_not(far[side]))
            def _(side=side):
                halo_copy(field, turn, 1, side).start()

        for side in range(2):

            @pl.when(sides[0][side])
            def _(side=side):
                halo_copy(field, turn, 0, side).start()

    def slots_copy(axis, side):
        index = 2 * axis + side
        if axis == 0:
            target = at_gx(gx + 1 if side else gx - 1)
        else:
            target = at_yz(yz + 1 if side else yz - 1)
        return pltpu.make_async_remote_copy(
            src_ref=slots,
            dst_ref=slots_beside.at[2 * axis + 1 - side],
            send_sem=slots_send.at[index],
            recv_sem=slots_recv.at[2 * axis + 1 - side],
            device_id=target,
            device_id_type=MESH,
        )

    def wait_slots(axis, side):
        index = 2 * axis + side
        pltpu.make_async_remote_copy(
            src_ref=slots,
            dst_ref=slots_beside.at[index],
            send_sem=slots_send.at[index],
            recv_sem=slots_recv.at[index],
            device_id=(cond, y, core, x, zl),
            device_id_type=MESH,
        ).wait_recv()

    def wait_faces(turn):
        def body(axis, side):
            pltpu.make_async_remote_copy(
                src_ref=(halo_x if axis == 0 else halo_y).at[turn, side],
                dst_ref=(halo_x if axis == 0 else halo_y).at[turn, side],
                send_sem=halo_send.at[turn, 2 * axis + side],
                recv_sem=halo_recv.at[turn, 2 * axis + side],
                device_id=(cond, y, core, x, zl),
                device_id_type=MESH,
            ).wait_recv()

        each_side(body)

    def drain_faces(field, turn):
        each_side(lambda axis, side: halo_copy(field, turn, axis, side).wait_send())

    tiles = [(r, c) for r in range(n_row) for c in range(n_col)]

    def window(block, r, c):
        at = block * span + (r * n_col + c) * SUBLANES
        return pl.ds(at if isinstance(at, int) else pl.multiple_of(at, SUBLANES), SUBLANES)

    def neighbours(field, block, lo, hi):
        sub = lax.broadcasted_iota(jnp.int32, (SUBLANES, LANES), 0)
        lane = lax.broadcasted_iota(jnp.int32, (SUBLANES, LANES), 1)
        zero = jnp.zeros((SUBLANES, LANES), jnp.float32)

        def tile_of(e, b, r, c):
            return field[e, window(b, r, c), :]

        total = [[None] * len(tiles) for _ in range(NVAR)]
        for e in range(NVAR):
            here = {rc: tile_of(e, block, *rc) for rc in tiles}
            terms = {}
            if hi:
                terms[X_HI] = {rc: tile_of(e, block + 1, *rc) for rc in tiles}
            if lo:
                terms[X_LO] = {rc: tile_of(e, block - 1, *rc) for rc in tiles}
            for d, shift, axis, index, edge in (
                (Y_HI, SUBLANES - 1, 0, sub, SUBLANES - 1),
                (Y_LO, 1, 0, sub, 0),
                (Z_HI, LANES - 1, 1, lane, LANES - 1),
                (Z_LO, 1, 1, lane, 0),
            ):
                turned = {rc: pltpu.roll(here[rc], shift, axis) for rc in tiles}
                step = 1 if edge else -1
                moved = {}
                for r, c in tiles:
                    beside = (r + step, c) if axis == 0 else (r, c + step)
                    moved[r, c] = jnp.where(index == edge, turned.get(beside, zero), turned[r, c])
                terms[d] = moved
            for d, values in terms.items():
                for k in range(NVAR):
                    coef = blocks[e, k, 0, d]
                    for i, rc in enumerate(tiles):
                        part = coef * values[rc]
                        total[k][i] = part if total[k][i] is None else total[k][i] + part
        return total

    def over_blocks(body):
        body(0, False, True)

        def inner(b, carry):
            body(b, True, True)
            return carry

        lax.fori_loop(1, nx - 1, inner, 0)
        body(nx - 1, True, False)

    def sweep(field, result):
        def body(block, lo, hi):
            total = neighbours(field, block, lo, hi)
            for i, rc in enumerate(tiles):
                at = window(block, *rc)
                scale = ratio[at, :]
                for k in range(NVAR):
                    result[k, at, :] = (1.0 - RELAX) * field[k, at, :] + scale * (
                        source[k, at, :] + total[k][i]
                    )

        over_blocks(body)

    def operate(field, result):
        def body(block, lo, hi):
            total = neighbours(field, block, lo, hi)
            for i, rc in enumerate(tiles):
                at = window(block, *rc)
                scale = diag[at, :]
                for k in range(NVAR):
                    result[k, at, :] = source[k, at, :] - scale * field[k, at, :] + total[k][i]

        over_blocks(body)

    def face_parts(axis, side):
        if axis == 0:
            first = (nx - 1) * span if side else 0
            return [(pl.ds(first + i, SUBLANES), pl.ds(i, SUBLANES)) for i in range(0, span, SUBLANES)]
        return [(line(side, c), pl.ds(c * nx, nx)) for c in range(n_col)]

    def add_halos(turn, result, scale):
        for axis, buffer in ((0, halo_x), (1, halo_y)):
            for side in range(2):
                d = (X_LO, X_HI, Y_LO, Y_HI)[2 * axis + side]
                for at, place in face_parts(axis, side):
                    factor = None if scale is None else scale[at, :]
                    outside = [buffer[turn, side, e, place, :] for e in range(NVAR)]
                    for k in range(NVAR):
                        part = blocks[0, k, 0, d] * outside[0]
                        for e in range(1, NVAR):
                            part = part + blocks[e, k, 0, d] * outside[e]
                        part = part if factor is None else factor * part
                        result[k, at, :] = result[k, at, :] + part

    load_start.wait()
    pack_faces(start, 0)
    pl.semaphore_wait(
        barrier, len(greeted) + step_up.astype(jnp.int32) + step_down.astype(jnp.int32)
    )
    send_faces(start, 0)

    for load in loads[6:]:
        load.wait()
    each_side(lambda axis, side: slots_copy(axis, side).start())
    for target in line_gx + [mirror]:
        pl.semaphore_signal(gate, inc=1, device_id=target, device_id_type=MESH)

    load_diag.wait()
    ratio[...] = RELAX / diag[...]
    load_mask.wait()
    load_sens.wait()
    for block in range(nx):
        for c in range(n_col):
            cols = pl.ds(c * LANES, LANES)
            for k in range(NVAR):
                weight = sens[k, pl.ds(block * ny, ny), cols].astype(jnp.float32)
                for r in range(n_row):
                    at = window(block, r, c)
                    mass[k, at, :] = (
                        surface_mask[at, :].astype(jnp.float32) * weight[r * SUBLANES : (r + 1) * SUBLANES]
                    )
    for axis, faces in ((1, face_y.at[3]), (0, face_x)):
        for side in range(2):
            d = (X_LO, X_HI, Y_LO, Y_HI)[2 * axis + side]
            for at, place in face_parts(axis, side):
                pull = [ratio[at, :] * mass[k, at, :] for k in range(NVAR)]
                for e in range(NVAR):
                    part = blocks[e, 0, 0, d] * pull[0]
                    for k in range(1, NVAR):
                        part = part + blocks[e, k, 0, d] * pull[k]
                    faces[side, e, place, :] = part
    send_faces(None, 3)

    load_source.wait()
    sweep(start, relaxed)

    def number_of(shape, dim):
        return lax.broadcasted_iota(jnp.int32, shape, dim)

    def lookup(table, pick, keep):
        spread = jnp.dot(
            table.astype(jnp.float32), pick.astype(jnp.float32), preferred_element_type=jnp.float32
        )
        return jnp.sum(jnp.where(keep, spread, 0.0), axis=0, keepdims=True)

    across, down = number_of((ny, rows), 1), number_of((ny, rows), 0)
    lane, first = number_of((nx, rows), 1), number_of((nx, rows), 0)
    slot_row = lookup(slots[...], lax.rem(across, ny) == down, lax.div(lane, ny) == first)
    each_side(wait_slots)
    beside_row = jnp.where(number_of((1, rows), 1) < 2 * (nx + ny), 0.0, -8.0)
    for side in range(2):
        base_lane = side * ny
        beside_row = beside_row + lookup(
            slots_beside[side],
            across - base_lane == down,
            first == (0 if side else nx - 1),
        )
        base_lane = 2 * ny + side * nx
        beside_row = beside_row + lookup(
            slots_beside[2 + side],
            down == (0 if side else ny - 1),
            lane - base_lane == first,
        )
    n_out = NDES // LANES
    number = number_of((3 * n_out, rows), 0)
    third = lax.div(number, n_out)
    wanted = 2 * lax.rem(number, n_out) + jnp.where(third == 0, 0, jnp.where(third == 1, -1, 1))
    onehot[:, :rows] = jnp.where(slot_row == wanted.astype(jnp.float32), 1.0, 0.0)
    onehot[:, rows:] = jnp.where(beside_row == wanted.astype(jnp.float32), 1.0, 0.0)
    surface[rows:, :] = jnp.zeros_like(surface[rows:, :])
    load_base.wait()

    wait_faces(0)
    add_halos(0, relaxed, ratio)
    pack_faces(relaxed, 1)
    send_faces(relaxed, 1)
    sweep(relaxed, smoothed)

    for block in range(nx):
        for r, c in tiles:
            at = window(block, r, c)
            part = [smoothed[k, at, :] * mass[k, at, :] for k in range(NVAR)]
            surface[pl.ds(block * ny + r * SUBLANES, SUBLANES), pl.ds(c * LANES, LANES)] = functools.reduce(
                jnp.add, part
            )
    wait_faces(3)
    for axis, buffer in ((0, halo_x), (1, halo_y)):
        for side in range(2):
            for i, (at, place) in enumerate(face_parts(axis, side)):
                part = [relaxed[e, at, :] * buffer[3, side, e, place, :] for e in range(NVAR)]
                if axis == 0:
                    to = rows + side * ny + (i // n_col) * SUBLANES
                    c = i % n_col
                else:
                    to = rows + 2 * ny + side * nx
                    c = i
                surface[pl.ds(to, SUBLANES), pl.ds(c * LANES, LANES)] = functools.reduce(jnp.add, part)
    projected = jnp.dot(
        surface[...], base[...], precision=lax.Precision.HIGHEST, preferred_element_type=jnp.float32
    )
    looked = jnp.dot(
        onehot[...], projected, precision=lax.Precision.HIGHEST, preferred_element_type=jnp.float32
    )
    even, before, after = (looked[i * n_out : (i + 1) * n_out] for i in range(3))
    half = lax.broadcasted_iota(jnp.int32, (n_out, LANES), 1) < LANES // 2
    swapped = pltpu.roll(jnp.where(half, after, before), LANES // 2, 1)
    whole = jnp.full((n_out, LANES), (weights[0] + weights[1]).astype(jnp.float32))
    mine = jnp.where(cond == 0, weights[0], weights[1]).astype(jnp.float32)
    scaled = (even + swapped) * (jnp.full((n_out, LANES), mine) / whole)
    outgoing[...] = scaled.reshape(n_out, 1, LANES)

    def plane_copy(target, number):
        return pltpu.make_async_remote_copy(
            src_ref=outgoing.at[number],
            dst_ref=plane_in.at[plane],
            send_sem=plane_send,
            recv_sem=plane_recv,
            device_id=target,
            device_id_type=MESH,
        )

    pl.semaphore_wait(gate, len(line_gx) + 1)
    for target, number in plane_targets:
        plane_copy(target, number).start()
    plane_in[plane] = outgoing[plane]


    wait_faces(1)
    add_halos(1, smoothed, ratio)
    pack_faces(smoothed, 2)
    send_faces(smoothed, 2)
    drain_faces(start, 0)
    drain_faces(None, 3)
    each_side(lambda axis, side: slots_copy(axis, side).wait_send())
    operate(smoothed, residual)
    drain_faces(relaxed, 1)

    everyone = pltpu.make_async_remote_copy(
        src_ref=outgoing.at[pl.ds(0, n_plane - 1)],
        dst_ref=plane_in.at[pl.ds(0, n_plane - 1)],
        send_sem=plane_send,
        recv_sem=plane_recv,
        device_id=(cond, y, core, x, zl),
        device_id_type=MESH,
    )
    everyone.wait_recv()
    row = plane_in[0]
    for i in range(1, n_plane):
        row = row + plane_in[i]
    row_out[0] = row
    column_in[z] = row

    def column_copy(i, target):
        return pltpu.make_async_remote_copy(
            src_ref=row_out.at[0],
            dst_ref=column_in.at[z],
            send_sem=column_send.at[i],
            recv_sem=column_recv,
            device_id=target,
            device_id_type=MESH,
        )

    for i, target in enumerate(z_targets):
        column_copy(i, target).start()

    wait_faces(2)
    add_halos(2, residual, None)
    everyone.wait_send()
    drain_faces(smoothed, 2)

    pltpu.make_async_remote_copy(
        src_ref=column_in.at[pl.ds(0, n_z - 1)],
        dst_ref=column_in.at[pl.ds(0, n_z - 1)],
        send_sem=column_send.at[0],
        recv_sem=column_recv,
        device_id=(cond, y, core, x, zl),
        device_id_type=MESH,
    ).wait_recv()
    row = column_in[0]
    for i in range(1, n_z):
        row = row + column_in[i]
    width = LANES // n_zl
    part = row[:, :width]
    for q in range(1, n_zl):
        part = jnp.where(zl == q, row[:, q * width : (q + 1) * width], part)
    gradient[...] = part
    for i, target in enumerate(z_targets):
        column_copy(i, target).wait_send()


def put_out(*refs):
    count = (len(refs) - 1) // 2
    copies = [pltpu.make_async_copy(refs[i], refs[count + i], refs[-1].at[i]) for i in range(count)]
    for copy in copies:
        copy.start()
    for copy in copies:
        copy.wait()


def to_tiles(array):
    *lead, ny, nz = array.shape
    split = array.reshape(*lead, ny // SUBLANES, SUBLANES, nz // LANES, LANES)
    return jnp.swapaxes(split, -2, -3).reshape(*lead[:-1], -1, LANES)


def from_tiles(array, shape):
    *lead, ny, nz = shape
    split = array.reshape(*lead, ny // SUBLANES, nz // LANES, SUBLANES, LANES)
    return jnp.swapaxes(split, -2, -3).reshape(shape)


def local(
    dims,
    adjoint,
    objective_gradient,
    diagonal,
    flux_blocks,
    flux_sensitivity,
    surface_mask,
    patch_band_slot,
    design_basis,
    condition_weights,
):
    _, nvar, nx, ny, nz = adjoint.shape
    rows = nx * ny
    n_cond, n_y, n_core, n_x, n_zl = dims
    n_plane, n_z = n_y * n_core * n_x, n_cond * n_zl
    f32 = jnp.float32
    flat = nx * ny * nz // LANES
    field, cell = (nvar, flat, LANES), (flat, LANES)
    hbm = pl.BlockSpec(memory_space=pltpu.HBM)
    vmem = pl.BlockSpec(memory_space=pltpu.VMEM)
    dma = pltpu.SemaphoreType.DMA
    smoothed, residual, gradient = pl.pallas_call(
        functools.partial(kernel, dims),
        out_shape=(
            jax.ShapeDtypeStruct(field, f32),
            jax.ShapeDtypeStruct(field, f32),
            jax.ShapeDtypeStruct((1, LANES // n_zl), f32),
        ),
        in_specs=[hbm] * 9,
        out_specs=(vmem, vmem, vmem),
        scratch_shapes=[
            pltpu.SMEM((nvar, nvar, 1, 6), f32),
            pltpu.SMEM((n_cond,), jnp.int32),
            pltpu.VMEM((nx, ny), jnp.int32),
            pltpu.VMEM(field, f32),
            pltpu.VMEM(field, f32),
            pltpu.VMEM(field, f32),
            pltpu.VMEM(cell, f32),
            pltpu.VMEM(cell, f32),
            pltpu.VMEM((nvar, rows, nz), jnp.bfloat16),
            pltpu.VMEM(cell, jnp.int32),
            pltpu.VMEM(design_basis.shape, f32),
            pltpu.VMEM((2 * rows, nz), f32),
            pltpu.VMEM((3 * NDES // LANES, 2 * rows), f32),
            pltpu.VMEM(field, f32),
            pltpu.VMEM((4, 2, nvar, ny * nz // LANES, LANES), f32),
            pltpu.VMEM((4, 2, nvar, nx * nz // LANES, LANES), f32),
            pltpu.VMEM((2, nvar, ny * nz // LANES, LANES), f32),
            pltpu.VMEM((4, 2, nvar, nx * nz // LANES, LANES), f32),
            pltpu.VMEM((4, nx, ny), jnp.int32),
            pltpu.VMEM((NDES // LANES, 1, LANES), f32),
            pltpu.VMEM((n_plane, 1, LANES), f32),
            pltpu.VMEM((1, 1, LANES), f32),
            pltpu.VMEM((n_z, 1, LANES), f32),
            dma((9,)),
            dma((4, 4)),
            dma((4, 4)),
            dma((4,)),
            dma((4,)),
            pltpu.SemaphoreType.REGULAR,
            dma,
            dma,
            dma((n_z - 1,)),
            dma,
        ],
        compiler_params=pltpu.CompilerParams(
            collective_id=0, has_side_effects=True, vmem_limit_bytes=KERNEL_VMEM
        ),
        name="adjoint_step",
    )(
        *(
            pltpu.with_memory_space_constraint(a, pltpu.HBM)
            for a in (
                to_tiles(adjoint[0]),
                to_tiles(objective_gradient[0]),
                to_tiles(diagonal),
                flux_sensitivity.reshape(nvar, rows, nz),
                to_tiles(surface_mask),
                design_basis,
                jnp.transpose(flux_blocks, (2, 3, 0, 1)),
                condition_weights,
                patch_band_slot,
            )
        )
    )
    results = (smoothed, residual, gradient)
    smoothed, residual, gradient = pl.pallas_call(
        put_out,
        out_shape=tuple(jax.ShapeDtypeStruct(a.shape, a.dtype) for a in results),
        in_specs=[vmem] * 3,
        out_specs=(hbm,) * 3,
        scratch_shapes=[dma((3,))],
        compiler_params=pltpu.CompilerParams(vmem_limit_bytes=4 * 1024 * 1024),
        name="put_out",
    )(*results)
    whole = (1, nvar, nx, ny, nz)
    return from_tiles(smoothed, whole), from_tiles(residual, whole), gradient.reshape(-1)


def solution(mesh):
    dims = (mesh.shape["cond"], 4, 2, 4, 4)
    torus = Mesh(mesh.devices.reshape(dims), AXES)
    in_specs = (
        P("cond", None, GX, YZ, None),
        P("cond", None, GX, YZ, None),
        P(GX, YZ, None),
        P("cond", None, None, None),
        P("cond", None, GX, YZ, None),
        P(GX, YZ, None),
        P(GX, YZ),
        P(),
        P(),
    )
    out_specs = (P("cond", None, GX, YZ, None), P("cond", None, GX, YZ, None), P(GX_YZ))
    return jax.shard_map(
        functools.partial(local, dims), mesh=torus, in_specs=in_specs, out_specs=out_specs, check_vma=False
    )
```

```python
import functools

import jax
import jax.numpy as jnp
from jax import lax
from jax.experimental import pallas as pl
from jax.experimental.pallas import tpu as pltpu
from jax.sharding import Mesh
from jax.sharding import PartitionSpec as P

NDES = 4096
NVAR = 5
LANES = 128
SUBLANES = 8
AXES = ("cond", "gx_0", "gx_1", "yz_0", "yz_1")
GX = ("gx_0", "gx_1")
YZ = ("yz_0", "yz_1")
GX_YZ = GX + YZ
MESH = pl.DeviceIdType.MESH
RELAX = 0.8
KERNEL_VMEM = 40 * 1024 * 1024
X_HI, X_LO, Y_HI, Y_LO, Z_HI, Z_LO = range(6)


def kernel(
    dims,
    adjoint,
    objective,
    diagonal,
    sensitivity,
    mask,
    basis,
    blocks_in,
    weights_in,
    slots_in,
    smoothed,
    residual,
    gradient,
    blocks,
    weights,
    slots,
    start,
    relaxed,
    source,
    diag,
    ratio,
    sens,
    surface_mask,
    base,
    surface,
    onehot,
    base_parts,
    mass,
    pulls,
    fixed,
    halo_x,
    halo_y,
    face_x,
    face_y,
    slots_beside,
    outgoing,
    plane_in,
    row_out,
    column_in,
    local_sem,
    halo_send,
    halo_recv,
    slots_send,
    slots_recv,
    gate,
    plane_send,
    plane_recv,
    column_send,
    column_recv,
):
    n_cond, n_y, n_core, n_x, n_zl = dims
    nx, ny = slots.shape
    rows = nx * ny
    n_row, n_col = ny // SUBLANES, basis.shape[0] // LANES
    span = n_row * n_col * SUBLANES
    n_gx, n_yz, n_plane, n_z = n_y * n_core, n_x * n_zl, n_y * n_core * n_x, n_cond * n_zl

    cond, y, core, x, zl = (lax.axis_index(a) for a in AXES)
    gx, yz = y * n_core + core, x * n_zl + zl
    plane, z = gx * n_x + x, cond * n_zl + zl

    def at_gx(g):
        return (cond, lax.div(g, n_core), lax.rem(g, n_core), x, zl)

    def at_yz(q):
        return (cond, y, core, lax.div(q, n_zl), lax.rem(q, n_zl))

    def around(index, size):
        return [index] + [lax.rem(index + o, size) for o in range(1, size)]

    conds, ys, cores, xs, zls = (around(i, n) for i, n in zip((cond, y, core, x, zl), dims))
    steps = [
        (i, j, k, l)
        for i in range(n_cond)
        for j in range(n_y)
        for k in range(n_x)
        for l in range(n_zl)
        if i or j or k or l
    ]
    steps.sort(key=lambda s: -(min(s[1], n_y - s[1]) + min(s[2], n_x - s[2]) + (n_zl if s[0] else s[3])))
    chip_targets = [
        ((conds[i], ys[j], core, xs[k], zls[l]), zls[l] * n_y * n_x + ys[j] * n_x + xs[k])
        for i, j, k, l in steps
    ]
    n_chips = len(steps) + 1
    chip = (cond * n_zl + zl) * n_y * n_x + y * n_x + x

    barrier = pltpu.get_barrier_semaphore()

    def greet(target):
        pl.semaphore_signal(barrier, inc=1, device_id=target, device_id_type=MESH)

    step_up = jnp.logical_and(zl == n_zl - 1, x < n_x - 1)
    step_down = jnp.logical_and(zl == 0, x > 0)

    @pl.when(step_up)
    def _():
        greet(at_yz(yz + 1))

    @pl.when(step_down)
    def _():
        greet(at_yz(yz - 1))

    line_gx = [(cond, b, c, x, zl) for i, b in enumerate(ys) for j, c in enumerate(cores) if i or j]
    mirror = (n_cond - 1 - cond, y, core, x, n_zl - 1 - zl)
    greeted = (
        line_gx + [(cond, y, core, d, zl) for d in xs[1:]] + [(cond, y, core, x, e) for e in zls[1:]] + [mirror]
    )
    for target in greeted:
        greet(target)

    pairs = (
        (adjoint, start),
        (diagonal, diag),
        (objective, source),
        (mask, surface_mask),
        (sensitivity, sens),
        (basis, base),
        (blocks_in, blocks),
        (weights_in, weights),
        (slots_in, slots),
    )
    loads = [pltpu.make_async_copy(a, b, local_sem.at[i]) for i, (a, b) in enumerate(pairs)]
    load_start, load_diag, load_source, load_mask, load_sens, load_base = loads[:6]
    for load in loads:
        load.start()

    sides = (
        (gx > 0, gx < n_gx - 1),
        (yz > 0, yz < n_yz - 1),
    )

    for axis, buffer in ((0, halo_x), (1, halo_y)):
        for side in range(2):

            @pl.when(jnp.logical_not(sides[axis][side]))
            def _(buffer=buffer, side=side, index=2 * axis + side):
                buffer[:, side] = jnp.zeros_like(buffer[:, side])
                slots_beside[index] = jnp.zeros_like(slots_beside[index])

    def halo_copy(field, turn, axis, side):
        index = 2 * axis + side
        if axis == 0:
            if field is None:
                src = face_x.at[side]
            else:
                src = field.at[:, pl.ds((nx - 1) * span if side else 0, span)]
            dst = halo_x.at[turn, 1 - side]
            target = at_gx(gx + 1 if side else gx - 1)
        else:
            src = face_y.at[turn, side]
            dst = halo_y.at[turn, 1 - side]
            target = at_yz(yz + 1 if side else yz - 1)
        return pltpu.make_async_remote_copy(
            src_ref=src,
            dst_ref=dst,
            send_sem=halo_send.at[turn, index],
            recv_sem=halo_recv.at[turn, 2 * axis + 1 - side],
            device_id=target,
            device_id_type=MESH,
        )

    def each_side(body):
        for axis in (1, 0):
            for side in range(2):

                @pl.when(sides[axis][side])
                def _(axis=axis, side=side):
                    body(axis, side)

    def line(side, c):
        first = ((n_row - 1) * n_col + c) * SUBLANES + SUBLANES - 1 if side else c * SUBLANES
        return pl.ds(first, nx, stride=span)

    def pack_faces(field, turn):
        for side in range(2):
            for e in range(NVAR):
                for c in range(n_col):
                    face_y[turn, side, e, pl.ds(c * nx, nx), :] = field[e, line(side, c), :]

    far = (zl == 0, zl == n_zl - 1)

    def send_faces(field, turn):
        for side in range(2):

            @pl.when(jnp.logical_and(sides[1][side], far[side]))
            def _(side=side):
                halo_copy(field, turn, 1, side).start()

        for side in range(2):

            @pl.when(jnp.logical_not(far[side]))
            def _(side=side):
                halo_copy(field, turn, 1, side).start()

        for side in range(2):

            @pl.when(sides[0][side])
            def _(side=side):
                halo_copy(field, turn, 0, side).start()

    def slots_copy(axis, side):
        index = 2 * axis + side
        if axis == 0:
            target = at_gx(gx + 1 if side else gx - 1)
        else:
            target = at_yz(yz + 1 if side else yz - 1)
        return pltpu.make_async_remote_copy(
            src_ref=slots,
            dst_ref=slots_beside.at[2 * axis + 1 - side],
            send_sem=slots_send.at[index],
            recv_sem=slots_recv.at[2 * axis + 1 - side],
            device_id=target,
            device_id_type=MESH,
        )

    def wait_slots(axis, side):
        index = 2 * axis + side
        pltpu.make_async_remote_copy(
            src_ref=slots,
            dst_ref=slots_beside.at[index],
            send_sem=slots_send.at[index],
            recv_sem=slots_recv.at[index],
            device_id=(cond, y, core, x, zl),
            device_id_type=MESH,
        ).wait_recv()

    def wait_faces(turn):
        def body(axis, side):
            pltpu.make_async_remote_copy(
                src_ref=(halo_x if axis == 0 else halo_y).at[turn, side],
                dst_ref=(halo_x if axis == 0 else halo_y).at[turn, side],
                send_sem=halo_send.at[turn, 2 * axis + side],
                recv_sem=halo_recv.at[turn, 2 * axis + side],
                device_id=(cond, y, core, x, zl),
                device_id_type=MESH,
            ).wait_recv()

        each_side(body)

    def drain_faces(field, turn):
        each_side(lambda axis, side: halo_copy(field, turn, axis, side).wait_send())

    tiles = [(r, c) for r in range(n_row) for c in range(n_col)]

    def window(block, r, c):
        at = block * span + (r * n_col + c) * SUBLANES
        return pl.ds(at if isinstance(at, int) else pl.multiple_of(at, SUBLANES), SUBLANES)

    def moved(here, d):
        axis, size, up = (0 if d in (Y_HI, Y_LO) else 1), (SUBLANES if d in (Y_HI, Y_LO) else LANES), d in (Y_HI, Z_HI)
        index = lax.broadcasted_iota(jnp.int32, (SUBLANES, LANES), axis)
        zero = jnp.zeros((SUBLANES, LANES), jnp.float32)
        edge, shift, step = (size - 1, size - 1, 1) if up else (0, 1, -1)
        turned = {rc: pltpu.roll(here[rc], shift, axis) for rc in tiles}
        return {
            (r, c): jnp.where(
                index == edge, turned.get((r + step, c) if axis == 0 else (r, c + step), zero), turned[r, c]
            )
            for r, c in tiles
        }

    def neighbours(field, block, lo, hi):
        def tile_of(e, b, r, c):
            return field[e, window(b, r, c), :]

        total = [[None] * len(tiles) for _ in range(NVAR)]
        for e in range(NVAR):
            here = {rc: tile_of(e, block, *rc) for rc in tiles}
            terms = {}
            if hi:
                terms[X_HI] = {rc: tile_of(e, block + 1, *rc) for rc in tiles}
            if lo:
                terms[X_LO] = {rc: tile_of(e, block - 1, *rc) for rc in tiles}
            for d in (Y_HI, Y_LO, Z_HI, Z_LO):
                terms[d] = moved(here, d)
            for d, values in terms.items():
                for k in range(NVAR):
                    coef = blocks[e, k, 0, d]
                    for i, rc in enumerate(tiles):
                        part = coef * values[rc]
                        total[k][i] = part if total[k][i] is None else total[k][i] + part
        return total

    def over_blocks(body, between=None):
        body(0, False, True)

        def inner(b, carry):
            body(b, True, True)
            return carry

        if between is None:
            lax.fori_loop(1, nx - 1, inner, 0)
        else:
            lax.fori_loop(1, nx - 2, inner, 0)
            between()
            lax.fori_loop(nx - 2, nx - 1, inner, 0)
        body(nx - 1, True, False)

    def sweep(field, result, between=None):
        def body(block, lo, hi):
            total = neighbours(field, block, lo, hi)
            for i, rc in enumerate(tiles):
                at = window(block, *rc)
                scale = ratio[at, :]
                for k in range(NVAR):
                    result[k, at, :] = (1.0 - RELAX) * field[k, at, :] + scale * (
                        source[k, at, :] + total[k][i]
                    )

        over_blocks(body, between)

    def operate(field, result):
        def body(block, lo, hi):
            total = neighbours(field, block, lo, hi)
            for i, rc in enumerate(tiles):
                at = window(block, *rc)
                scale = diag[at, :]
                for k in range(NVAR):
                    result[k, at, :] = source[k, at, :] - scale * field[k, at, :] + total[k][i]

        over_blocks(body)

    def face_parts(axis, side):
        if axis == 0:
            first = (nx - 1) * span if side else 0
            return [(pl.ds(first + i, SUBLANES), pl.ds(i, SUBLANES)) for i in range(0, span, SUBLANES)]
        return [(line(side, c), pl.ds(c * nx, nx)) for c in range(n_col)]

    def add_halos(turn, result, scale):
        for axis, buffer in ((0, halo_x), (1, halo_y)):
            for side in range(2):
                d = (X_LO, X_HI, Y_LO, Y_HI)[2 * axis + side]
                for at, place in face_parts(axis, side):
                    factor = None if scale is None else scale[at, :]
                    outside = [buffer[turn, side, e, place, :] for e in range(NVAR)]
                    for k in range(NVAR):
                        part = blocks[0, k, 0, d] * outside[0]
                        for e in range(1, NVAR):
                            part = part + blocks[e, k, 0, d] * outside[e]
                        part = part if factor is None else factor * part
                        result[k, at, :] = result[k, at, :] + part

    load_start.wait()
    pack_faces(start, 0)
    for load in loads[6:]:
        load.wait()
    load_diag.wait()
    ratio[...] = RELAX / diag[...]
    load_mask.wait()
    load_sens.wait()
    for block in range(nx):
        for c in range(n_col):
            cols = pl.ds(c * LANES, LANES)
            for k in range(NVAR):
                weight = sens[k, pl.ds(block * ny, ny), cols].astype(jnp.float32)
                for r in range(n_row):
                    at = window(block, r, c)
                    mass[k, at, :] = (
                        surface_mask[at, :].astype(jnp.float32) * weight[r * SUBLANES : (r + 1) * SUBLANES]
                    )
    for axis, faces in ((1, face_y.at[3]), (0, face_x)):
        for side in range(2):
            d = (X_LO, X_HI, Y_LO, Y_HI)[2 * axis + side]
            for at, place in face_parts(axis, side):
                pull = [ratio[at, :] * mass[k, at, :] for k in range(NVAR)]
                for e in range(NVAR):
                    part = blocks[e, 0, 0, d] * pull[0]
                    for k in range(1, NVAR):
                        part = part + blocks[e, k, 0, d] * pull[k]
                    faces[side, e, place, :] = part
    pl.semaphore_wait(
        barrier, len(greeted) + step_up.astype(jnp.int32) + step_down.astype(jnp.int32)
    )
    send_faces(start, 0)
    each_side(lambda axis, side: slots_copy(axis, side).start())
    line_zl = [(cond, y, core, x, e) for e in zls[1:]]

    def open_gate(i, targets):
        for target in targets:
            pl.semaphore_signal(gate.at[i], inc=1, device_id=target, device_id_type=MESH)

    open_gate(0, line_gx)

    send_faces(None, 3)

    load_source.wait()

    def second_gate():
        pl.semaphore_wait(gate.at[0], len(line_gx))
        open_gate(1, line_zl)

    sweep(start, relaxed, second_gate)

    def weigh(block, carry):
        pull = []
        for k in range(NVAR):
            pull.append({rc: ratio[window(block, *rc), :] * mass[k, window(block, *rc), :] for rc in tiles})
        for rc in tiles:
            at = window(block, *rc)
            part = [pull[k][rc] * source[k, at, :] for k in range(NVAR)]
            fixed[at, :] = functools.reduce(jnp.add, part)
        for d in range(6):
            for e in range(NVAR):
                line_of = {}
                for rc in tiles:
                    part = blocks[e, 0, 0, d] * pull[0][rc]
                    for k in range(1, NVAR):
                        part = part + blocks[e, k, 0, d] * pull[k][rc]
                    line_of[rc] = part
                if d in (Y_HI, Y_LO, Z_HI, Z_LO):
                    line_of = moved(line_of, {Y_HI: Y_LO, Y_LO: Y_HI, Z_HI: Z_LO, Z_LO: Z_HI}[d])
                for rc in tiles:
                    pulls[d, e, window(block, *rc), :] = line_of[rc]
        return carry

    lax.fori_loop(0, nx, weigh, 0)
    pl.semaphore_wait(gate.at[1], len(line_zl))
    open_gate(2, [mirror])

    def two_parts(value):
        high = value.astype(jnp.bfloat16)
        return high, (value - high.astype(jnp.float32)).astype(jnp.bfloat16)

    def multiply(a, b):
        return jnp.dot(a, b, preferred_element_type=jnp.float32)

    def number_of(shape, dim):
        return lax.broadcasted_iota(jnp.int32, shape, dim)

    def lookup(table, pick, keep):
        spread = jnp.dot(
            table.astype(jnp.float32), pick.astype(jnp.float32), preferred_element_type=jnp.float32
        )
        return jnp.sum(jnp.where(keep, spread, 0.0), axis=0, keepdims=True)

    across, down = number_of((ny, rows), 1), number_of((ny, rows), 0)
    lane, first = number_of((nx, rows), 1), number_of((nx, rows), 0)
    slot_row = lookup(slots[...], lax.rem(across, ny) == down, lax.div(lane, ny) == first)
    each_side(wait_slots)
    beside_row = jnp.where(number_of((1, rows), 1) < 2 * (nx + ny), 0.0, -8.0)
    for side in range(2):
        base_lane = side * ny
        beside_row = beside_row + lookup(
            slots_beside[side],
            across - base_lane == down,
            first == (0 if side else nx - 1),
        )
        base_lane = 2 * ny + side * nx
        beside_row = beside_row + lookup(
            slots_beside[2 + side],
            down == (0 if side else ny - 1),
            lane - base_lane == first,
        )
    n_out = NDES // LANES
    number = number_of((3 * n_out, rows), 0)
    third = lax.div(number, n_out)
    place = lax.rem(number, n_out)
    half_out = n_out // n_core
    row_of = (lax.div(lax.rem(place, half_out), n_x) * n_core + lax.div(place, half_out)) * n_x + lax.rem(place, n_x)
    wanted = 2 * row_of + jnp.where(third == 0, 0, jnp.where(third == 1, -1, 1))
    onehot[:, :rows] = jnp.where(slot_row == wanted.astype(jnp.float32), 1.0, 0.0).astype(jnp.bfloat16)
    onehot[:, rows:] = jnp.where(beside_row == wanted.astype(jnp.float32), 1.0, 0.0).astype(jnp.bfloat16)
    surface[rows:, :] = jnp.zeros_like(surface[rows:, :])
    load_base.wait()
    base_parts[0], base_parts[1] = two_parts(base[...])

    wait_faces(0)
    add_halos(0, relaxed, ratio)
    pack_faces(relaxed, 1)
    send_faces(relaxed, 1)
    def add_surface(block, lo, hi):
        total = {}
        for rc in tiles:
            at = window(block, *rc)
            part = [fixed[at, :]]
            part += [(1.0 - RELAX) * mass[e, at, :] * relaxed[e, at, :] for e in range(NVAR)]
            for d, exists, step in ((X_HI, hi, 1), (X_LO, lo, -1)):
                if exists:
                    part += [pulls[d, e, at, :] * relaxed[e, window(block + step, *rc), :] for e in range(NVAR)]
            total[rc] = functools.reduce(jnp.add, part)
        for d in (Y_HI, Y_LO, Z_HI, Z_LO):
            line_of = {}
            for rc in tiles:
                at = window(block, *rc)
                part = [pulls[d, e, at, :] * relaxed[e, at, :] for e in range(NVAR)]
                line_of[rc] = functools.reduce(jnp.add, part)
            line_of = moved(line_of, d)
            total = {rc: total[rc] + line_of[rc] for rc in tiles}
        for r, c in tiles:
            at = block * ny + r * SUBLANES
            at = at if isinstance(at, int) else pl.multiple_of(at, SUBLANES)
            surface[pl.ds(at, SUBLANES), pl.ds(c * LANES, LANES)] = total[r, c]

    over_blocks(add_surface)
    wait_faces(3)
    for axis, buffer in ((0, halo_x), (1, halo_y)):
        for side in range(2):
            for i, (at, place) in enumerate(face_parts(axis, side)):
                part = [relaxed[e, at, :] * buffer[3, side, e, place, :] for e in range(NVAR)]
                if axis == 0:
                    to = rows + side * ny + (i // n_col) * SUBLANES
                    c = i % n_col
                else:
                    to = rows + 2 * ny + side * nx
                    c = i
                surface[pl.ds(to, SUBLANES), pl.ds(c * LANES, LANES)] = functools.reduce(jnp.add, part)
    high, low = two_parts(surface[...])
    projected = (
        multiply(high, base_parts[1]) + multiply(low, base_parts[0])
    ) + multiply(high, base_parts[0])
    high, low = two_parts(projected)
    looked = multiply(onehot[...], high) + multiply(onehot[...], low)
    even, before, after = (looked[i * n_out : (i + 1) * n_out] for i in range(3))
    half = lax.broadcasted_iota(jnp.int32, (n_out, LANES), 1) < LANES // 2
    swapped = pltpu.roll(jnp.where(half, after, before), LANES // 2, 1)
    whole = jnp.full((n_out, LANES), (weights[0] + weights[1]).astype(jnp.float32))
    mine = jnp.where(cond == 0, weights[0], weights[1]).astype(jnp.float32)
    scaled = (even + swapped) * (jnp.full((n_out, LANES), mine) / whole)
    outgoing[...] = scaled.reshape(n_out, 1, LANES)

    half = pl.ds(core * half_out, half_out)
    other = pl.ds((1 - core) * half_out, half_out)
    pair = pltpu.make_async_remote_copy(
        src_ref=outgoing.at[other],
        dst_ref=plane_in,
        send_sem=plane_send,
        recv_sem=plane_recv,
        device_id=(cond, y, 1 - core, x, zl),
        device_id_type=MESH,
    )
    pair.start()
    pl.semaphore_wait(gate.at[2], 1)
    pair.wait()
    width = LANES // n_zl
    summed = (outgoing[half] + plane_in[...]).reshape(half_out, LANES)
    for q in range(n_zl):
        quarter = summed if q == 0 else pltpu.roll(summed, LANES - q * width, 1)
        row_out[pl.ds(q * half_out, half_out)] = quarter[:, :width].reshape(half_out, 1, width)

    def chip_copy(target, number):
        return pltpu.make_async_remote_copy(
            src_ref=row_out.at[number],
            dst_ref=column_in.at[chip],
            send_sem=column_send,
            recv_sem=column_recv,
            device_id=target,
            device_id_type=MESH,
        )

    for target, number in chip_targets:
        chip_copy(target, number).start()
    column_in[chip] = row_out[zl * n_y * n_x + y * n_x + x]
    sweep(relaxed, smoothed)

    wait_faces(1)
    add_halos(1, smoothed, ratio)
    pack_faces(smoothed, 2)
    send_faces(smoothed, 2)
    drain_faces(start, 0)
    drain_faces(None, 3)
    each_side(lambda axis, side: slots_copy(axis, side).wait_send())
    operate(smoothed, residual)
    drain_faces(relaxed, 1)

    wait_faces(2)
    add_halos(2, residual, None)
    drain_faces(smoothed, 2)

    everyone = pltpu.make_async_remote_copy(
        src_ref=column_in.at[pl.ds(0, n_chips - 1)],
        dst_ref=column_in.at[pl.ds(0, n_chips - 1)],
        send_sem=column_send,
        recv_sem=column_recv,
        device_id=(cond, y, core, x, zl),
        device_id_type=MESH,
    )
    everyone.wait_recv()
    groups = 8
    sums = [column_in[i] for i in range(groups)]
    for i in range(groups, n_chips):
        sums[i % groups] = sums[i % groups] + column_in[i]
    row = functools.reduce(jnp.add, sums)
    gradient[...] = row
    everyone.wait_send()


def put_out(*refs):
    count = (len(refs) - 1) // 2
    copies = [pltpu.make_async_copy(refs[i], refs[count + i], refs[-1].at[i]) for i in range(count)]
    for copy in copies:
        copy.start()
    for copy in copies:
        copy.wait()


def to_tiles(array):
    *lead, ny, nz = array.shape
    split = array.reshape(*lead, ny // SUBLANES, SUBLANES, nz // LANES, LANES)
    return jnp.swapaxes(split, -2, -3).reshape(*lead[:-1], -1, LANES)


def from_tiles(array, shape):
    *lead, ny, nz = shape
    split = array.reshape(*lead, ny // SUBLANES, nz // LANES, SUBLANES, LANES)
    return jnp.swapaxes(split, -2, -3).reshape(shape)


def local(
    dims,
    adjoint,
    objective_gradient,
    diagonal,
    flux_blocks,
    flux_sensitivity,
    surface_mask,
    patch_band_slot,
    design_basis,
    condition_weights,
):
    _, nvar, nx, ny, nz = adjoint.shape
    rows = nx * ny
    n_cond, n_y, n_core, n_x, n_zl = dims
    n_plane, n_z = n_y * n_core * n_x, n_cond * n_zl
    f32 = jnp.float32
    flat = nx * ny * nz // LANES
    field, cell = (nvar, flat, LANES), (flat, LANES)
    hbm = pl.BlockSpec(memory_space=pltpu.HBM)
    vmem = pl.BlockSpec(memory_space=pltpu.VMEM)
    dma = pltpu.SemaphoreType.DMA
    smoothed, residual, gradient = pl.pallas_call(
        functools.partial(kernel, dims),
        out_shape=(
            jax.ShapeDtypeStruct(field, f32),
            jax.ShapeDtypeStruct(field, f32),
            jax.ShapeDtypeStruct((1, LANES // n_zl), f32),
        ),
        in_specs=[hbm] * 9,
        out_specs=(vmem, vmem, vmem),
        scratch_shapes=[
            pltpu.SMEM((nvar, nvar, 1, 6), f32),
            pltpu.SMEM((n_cond,), jnp.int32),
            pltpu.VMEM((nx, ny), jnp.int32),
            pltpu.VMEM(field, f32),
            pltpu.VMEM(field, f32),
            pltpu.VMEM(field, f32),
            pltpu.VMEM(cell, f32),
            pltpu.VMEM(cell, f32),
            pltpu.VMEM((nvar, rows, nz), jnp.bfloat16),
            pltpu.VMEM(cell, jnp.int32),
            pltpu.VMEM(design_basis.shape, f32),
            pltpu.VMEM((2 * rows, nz), f32),
            pltpu.VMEM((3 * NDES // LANES, 2 * rows), jnp.bfloat16),
            pltpu.VMEM((2, *design_basis.shape), jnp.bfloat16),
            pltpu.VMEM(field, f32),
            pltpu.VMEM((6, *field), f32),
            pltpu.VMEM(cell, f32),
            pltpu.VMEM((4, 2, nvar, ny * nz // LANES, LANES), f32),
            pltpu.VMEM((4, 2, nvar, nx * nz // LANES, LANES), f32),
            pltpu.VMEM((2, nvar, ny * nz // LANES, LANES), f32),
            pltpu.VMEM((4, 2, nvar, nx * nz // LANES, LANES), f32),
            pltpu.VMEM((4, nx, ny), jnp.int32),
            pltpu.VMEM((NDES // LANES, 1, LANES), f32),
            pltpu.VMEM((n_y * n_x, 1, LANES), f32),
            pltpu.VMEM((n_zl * n_y * n_x, 1, LANES // n_zl), f32),
            pltpu.VMEM((n_cond * n_zl * n_y * n_x, 1, LANES // n_zl), f32),
            dma((9,)),
            dma((4, 4)),
            dma((4, 4)),
            dma((4,)),
            dma((4,)),
            pltpu.SemaphoreType.REGULAR((3,)),
            dma,
            dma,
            dma,
            dma,
        ],
        compiler_params=pltpu.CompilerParams(
            collective_id=0, has_side_effects=True, vmem_limit_bytes=KERNEL_VMEM
        ),
        name="adjoint_step",
    )(
        *(
            pltpu.with_memory_space_constraint(a, pltpu.HBM)
            for a in (
                to_tiles(adjoint[0]),
                to_tiles(objective_gradient[0]),
                to_tiles(diagonal),
                flux_sensitivity.reshape(nvar, rows, nz),
                to_tiles(surface_mask),
                design_basis,
                jnp.transpose(flux_blocks, (2, 3, 0, 1)),
                condition_weights,
                patch_band_slot,
            )
        )
    )
    results = (smoothed, residual, gradient)
    smoothed, residual, gradient = pl.pallas_call(
        put_out,
        out_shape=tuple(jax.ShapeDtypeStruct(a.shape, a.dtype) for a in results),
        in_specs=[vmem] * 3,
        out_specs=(hbm,) * 3,
        scratch_shapes=[dma((3,))],
        compiler_params=pltpu.CompilerParams(vmem_limit_bytes=4 * 1024 * 1024),
        name="put_out",
    )(*results)
    whole = (1, nvar, nx, ny, nz)
    return from_tiles(smoothed, whole), from_tiles(residual, whole), gradient.reshape(-1)


def solution(mesh):
    dims = (mesh.shape["cond"], 4, 2, 4, 4)
    torus = Mesh(mesh.devices.reshape(dims), AXES)
    in_specs = (
        P("cond", None, GX, YZ, None),
        P("cond", None, GX, YZ, None),
        P(GX, YZ, None),
        P("cond", None, None, None),
        P("cond", None, GX, YZ, None),
        P(GX, YZ, None),
        P(GX, YZ),
        P(),
        P(),
    )
    out_specs = (P("cond", None, GX, YZ, None), P("cond", None, GX, YZ, None), P(GX_YZ))
    return jax.shard_map(
        functools.partial(local, dims), mesh=torus, in_specs=in_specs, out_specs=out_specs, check_vma=False
    )
```

```python
import functools

import jax
import jax.numpy as jnp
from jax import lax
from jax.experimental import pallas as pl
from jax.experimental.pallas import tpu as pltpu
from jax.sharding import Mesh
from jax.sharding import PartitionSpec as P

NDES = 4096
NVAR = 5
LANES = 128
SUBLANES = 8
AXES = ("cond", "gx_0", "gx_1", "yz_0", "yz_1")
GX = ("gx_0", "gx_1")
YZ = ("yz_0", "yz_1")
GX_YZ = GX + YZ
MESH = pl.DeviceIdType.MESH
RELAX = 0.8
KERNEL_VMEM = 40 * 1024 * 1024
X_HI, X_LO, Y_HI, Y_LO, Z_HI, Z_LO = range(6)


def kernel(
    dims,
    adjoint,
    objective,
    diagonal,
    sensitivity,
    mask,
    basis,
    blocks_in,
    weights_in,
    slots_in,
    smoothed,
    residual,
    gradient,
    blocks,
    weights,
    slots,
    start,
    relaxed,
    source,
    diag,
    ratio,
    sens,
    surface_mask,
    base,
    surface,
    onehot,
    base_parts,
    mass,
    pulls,
    fixed,
    halo_x,
    halo_y,
    face_x,
    face_y,
    slots_beside,
    row_out,
    column_in,
    local_sem,
    halo_send,
    halo_recv,
    slots_send,
    slots_recv,
    gate,
    column_send,
    column_recv,
):
    n_cond, n_y, n_core, n_x, n_zl = dims
    nx, ny = slots.shape
    rows = nx * ny
    n_row, n_col = ny // SUBLANES, basis.shape[0] // LANES
    span = n_row * n_col * SUBLANES
    n_gx, n_yz, n_plane, n_z = n_y * n_core, n_x * n_zl, n_y * n_core * n_x, n_cond * n_zl

    cond, y, core, x, zl = (lax.axis_index(a) for a in AXES)
    gx, yz = y * n_core + core, x * n_zl + zl
    plane, z = gx * n_x + x, cond * n_zl + zl

    def at_gx(g):
        return (cond, lax.div(g, n_core), lax.rem(g, n_core), x, zl)

    def at_yz(q):
        return (cond, y, core, lax.div(q, n_zl), lax.rem(q, n_zl))

    def around(index, size):
        return [index] + [lax.rem(index + o, size) for o in range(1, size)]

    conds, ys, cores, xs, zls = (around(i, n) for i, n in zip((cond, y, core, x, zl), dims))
    steps = [
        (i, j, c, k, l)
        for i in range(n_cond)
        for j in range(n_y)
        for c in range(n_core)
        for k in range(n_x)
        for l in range(n_zl)
        if i or j or c or k or l
    ]
    steps.sort(key=lambda s: -(min(s[1], n_y - s[1]) + min(s[3], n_x - s[3]) + (n_zl if s[0] else s[4])))

    def piece_of(b, c, d, e):
        return ((e * n_core + c) * n_y + b) * n_x + d

    all_targets = [
        ((conds[i], ys[j], cores[c], xs[k], zls[l]), piece_of(ys[j], cores[c], xs[k], zls[l]))
        for i, j, c, k, l in steps
    ]
    n_devices = len(steps) + 1
    own_piece = piece_of(y, core, x, zl)
    device = cond * (n_devices // n_cond) + own_piece

    barrier = pltpu.get_barrier_semaphore()

    def greet(target):
        pl.semaphore_signal(barrier, inc=1, device_id=target, device_id_type=MESH)

    step_up = jnp.logical_and(zl == n_zl - 1, x < n_x - 1)
    step_down = jnp.logical_and(zl == 0, x > 0)

    @pl.when(step_up)
    def _():
        greet(at_yz(yz + 1))

    @pl.when(step_down)
    def _():
        greet(at_yz(yz - 1))

    line_gx = [(cond, b, c, x, zl) for i, b in enumerate(ys) for j, c in enumerate(cores) if i or j]
    mirror = (n_cond - 1 - cond, y, core, x, n_zl - 1 - zl)
    greeted = (
        line_gx + [(cond, y, core, d, zl) for d in xs[1:]] + [(cond, y, core, x, e) for e in zls[1:]] + [mirror]
    )
    for target in greeted:
        greet(target)

    pairs = (
        (adjoint, start),
        (diagonal, diag),
        (objective, source),
        (mask, surface_mask),
        (sensitivity, sens),
        (basis, base),
        (blocks_in, blocks),
        (weights_in, weights),
        (slots_in, slots),
    )
    loads = [pltpu.make_async_copy(a, b, local_sem.at[i]) for i, (a, b) in enumerate(pairs)]
    load_start, load_diag, load_source, load_mask, load_sens, load_base = loads[:6]
    for load in loads:
        load.start()

    sides = (
        (gx > 0, gx < n_gx - 1),
        (yz > 0, yz < n_yz - 1),
    )

    for axis, buffer in ((0, halo_x), (1, halo_y)):
        for side in range(2):

            @pl.when(jnp.logical_not(sides[axis][side]))
            def _(buffer=buffer, side=side, index=2 * axis + side):
                buffer[:, side] = jnp.zeros_like(buffer[:, side])
                slots_beside[index] = jnp.zeros_like(slots_beside[index])

    def halo_copy(field, turn, axis, side):
        index = 2 * axis + side
        if axis == 0:
            if field is None:
                src = face_x.at[side]
            else:
                src = field.at[:, pl.ds((nx - 1) * span if side else 0, span)]
            dst = halo_x.at[turn, 1 - side]
            target = at_gx(gx + 1 if side else gx - 1)
        else:
            src = face_y.at[turn, side]
            dst = halo_y.at[turn, 1 - side]
            target = at_yz(yz + 1 if side else yz - 1)
        return pltpu.make_async_remote_copy(
            src_ref=src,
            dst_ref=dst,
            send_sem=halo_send.at[turn, index],
            recv_sem=halo_recv.at[turn, 2 * axis + 1 - side],
            device_id=target,
            device_id_type=MESH,
        )

    def each_side(body):
        for axis in (1, 0):
            for side in range(2):

                @pl.when(sides[axis][side])
                def _(axis=axis, side=side):
                    body(axis, side)

    def line(side, c):
        first = ((n_row - 1) * n_col + c) * SUBLANES + SUBLANES - 1 if side else c * SUBLANES
        return pl.ds(first, nx, stride=span)

    def pack_faces(field, turn):
        for side in range(2):
            for e in range(NVAR):
                for c in range(n_col):
                    face_y[turn, side, e, pl.ds(c * nx, nx), :] = field[e, line(side, c), :]

    far = (zl == 0, zl == n_zl - 1)

    def send_faces(field, turn):
        for side in range(2):

            @pl.when(jnp.logical_and(sides[1][side], far[side]))
            def _(side=side):
                halo_copy(field, turn, 1, side).start()

        for side in range(2):

            @pl.when(jnp.logical_not(far[side]))
            def _(side=side):
                halo_copy(field, turn, 1, side).start()

        for side in range(2):

            @pl.when(sides[0][side])
            def _(side=side):
                halo_copy(field, turn, 0, side).start()

    def slots_copy(axis, side):
        index = 2 * axis + side
        if axis == 0:
            target = at_gx(gx + 1 if side else gx - 1)
        else:
            target = at_yz(yz + 1 if side else yz - 1)
        return pltpu.make_async_remote_copy(
            src_ref=slots,
            dst_ref=slots_beside.at[2 * axis + 1 - side],
            send_sem=slots_send.at[index],
            recv_sem=slots_recv.at[2 * axis + 1 - side],
            device_id=target,
            device_id_type=MESH,
        )

    def wait_slots(axis, side):
        index = 2 * axis + side
        pltpu.make_async_remote_copy(
            src_ref=slots,
            dst_ref=slots_beside.at[index],
            send_sem=slots_send.at[index],
            recv_sem=slots_recv.at[index],
            device_id=(cond, y, core, x, zl),
            device_id_type=MESH,
        ).wait_recv()

    def wait_faces(turn):
        def body(axis, side):
            pltpu.make_async_remote_copy(
                src_ref=(halo_x if axis == 0 else halo_y).at[turn, side],
                dst_ref=(halo_x if axis == 0 else halo_y).at[turn, side],
                send_sem=halo_send.at[turn, 2 * axis + side],
                recv_sem=halo_recv.at[turn, 2 * axis + side],
                device_id=(cond, y, core, x, zl),
                device_id_type=MESH,
            ).wait_recv()

        each_side(body)

    def drain_faces(field, turn):
        each_side(lambda axis, side: halo_copy(field, turn, axis, side).wait_send())

    tiles = [(r, c) for r in range(n_row) for c in range(n_col)]

    def window(block, r, c):
        at = block * span + (r * n_col + c) * SUBLANES
        return pl.ds(at if isinstance(at, int) else pl.multiple_of(at, SUBLANES), SUBLANES)

    def moved(here, d):
        axis, size, up = (0 if d in (Y_HI, Y_LO) else 1), (SUBLANES if d in (Y_HI, Y_LO) else LANES), d in (Y_HI, Z_HI)
        index = lax.broadcasted_iota(jnp.int32, (SUBLANES, LANES), axis)
        zero = jnp.zeros((SUBLANES, LANES), jnp.float32)
        edge, shift, step = (size - 1, size - 1, 1) if up else (0, 1, -1)
        turned = {rc: pltpu.roll(here[rc], shift, axis) for rc in tiles}
        return {
            (r, c): jnp.where(
                index == edge, turned.get((r + step, c) if axis == 0 else (r, c + step), zero), turned[r, c]
            )
            for r, c in tiles
        }

    def neighbours(field, block, lo, hi):
        def tile_of(e, b, r, c):
            return field[e, window(b, r, c), :]

        total = [[None] * len(tiles) for _ in range(NVAR)]
        for e in range(NVAR):
            here = {rc: tile_of(e, block, *rc) for rc in tiles}
            terms = {}
            if hi:
                terms[X_HI] = {rc: tile_of(e, block + 1, *rc) for rc in tiles}
            if lo:
                terms[X_LO] = {rc: tile_of(e, block - 1, *rc) for rc in tiles}
            for d in (Y_HI, Y_LO, Z_HI, Z_LO):
                terms[d] = moved(here, d)
            for d, values in terms.items():
                for k in range(NVAR):
                    coef = blocks[e, k, 0, d]
                    for i, rc in enumerate(tiles):
                        part = coef * values[rc]
                        total[k][i] = part if total[k][i] is None else total[k][i] + part
        return total

    def over_blocks(body, between=None):
        body(0, False, True)

        def inner(b, carry):
            body(b, True, True)
            return carry

        if between is None:
            lax.fori_loop(1, nx - 1, inner, 0)
        else:
            lax.fori_loop(1, nx - 2, inner, 0)
            between()
            lax.fori_loop(nx - 2, nx - 1, inner, 0)
        body(nx - 1, True, False)

    def sweep(field, result, between=None):
        def body(block, lo, hi):
            total = neighbours(field, block, lo, hi)
            for i, rc in enumerate(tiles):
                at = window(block, *rc)
                scale = ratio[at, :]
                for k in range(NVAR):
                    result[k, at, :] = (1.0 - RELAX) * field[k, at, :] + scale * (
                        source[k, at, :] + total[k][i]
                    )

        over_blocks(body, between)

    def operate(field, result):
        def body(block, lo, hi):
            total = neighbours(field, block, lo, hi)
            for i, rc in enumerate(tiles):
                at = window(block, *rc)
                scale = diag[at, :]
                for k in range(NVAR):
                    result[k, at, :] = source[k, at, :] - scale * field[k, at, :] + total[k][i]

        over_blocks(body)

    def face_parts(axis, side):
        if axis == 0:
            first = (nx - 1) * span if side else 0
            return [(pl.ds(first + i, SUBLANES), pl.ds(i, SUBLANES)) for i in range(0, span, SUBLANES)]
        return [(line(side, c), pl.ds(c * nx, nx)) for c in range(n_col)]

    def add_halos(turn, result, scale):
        for axis, buffer in ((0, halo_x), (1, halo_y)):
            for side in range(2):
                d = (X_LO, X_HI, Y_LO, Y_HI)[2 * axis + side]
                for at, place in face_parts(axis, side):
                    factor = None if scale is None else scale[at, :]
                    outside = [buffer[turn, side, e, place, :] for e in range(NVAR)]
                    for k in range(NVAR):
                        part = blocks[0, k, 0, d] * outside[0]
                        for e in range(1, NVAR):
                            part = part + blocks[e, k, 0, d] * outside[e]
                        part = part if factor is None else factor * part
                        result[k, at, :] = result[k, at, :] + part

    load_start.wait()
    pack_faces(start, 0)
    for load in loads[6:]:
        load.wait()
    load_diag.wait()
    ratio[...] = RELAX / diag[...]
    load_mask.wait()
    load_sens.wait()
    for block in range(nx):
        for c in range(n_col):
            cols = pl.ds(c * LANES, LANES)
            for k in range(NVAR):
                weight = sens[k, pl.ds(block * ny, ny), cols].astype(jnp.float32)
                for r in range(n_row):
                    at = window(block, r, c)
                    mass[k, at, :] = (
                        surface_mask[at, :].astype(jnp.float32) * weight[r * SUBLANES : (r + 1) * SUBLANES]
                    )
    for axis, faces in ((1, face_y.at[3]), (0, face_x)):
        for side in range(2):
            d = (X_LO, X_HI, Y_LO, Y_HI)[2 * axis + side]
            for at, place in face_parts(axis, side):
                pull = [ratio[at, :] * mass[k, at, :] for k in range(NVAR)]
                for e in range(NVAR):
                    part = blocks[e, 0, 0, d] * pull[0]
                    for k in range(1, NVAR):
                        part = part + blocks[e, k, 0, d] * pull[k]
                    faces[side, e, place, :] = part
    pl.semaphore_wait(
        barrier, len(greeted) + step_up.astype(jnp.int32) + step_down.astype(jnp.int32)
    )
    send_faces(start, 0)
    each_side(lambda axis, side: slots_copy(axis, side).start())
    line_zl = [(cond, y, core, x, e) for e in zls[1:]]

    def open_gate(i, targets):
        for target in targets:
            pl.semaphore_signal(gate.at[i], inc=1, device_id=target, device_id_type=MESH)

    open_gate(0, line_gx)


    load_source.wait()

    def second_gate():
        pl.semaphore_wait(gate.at[0], len(line_gx))
        open_gate(1, line_zl)

    sweep(start, relaxed, second_gate)
    send_faces(None, 3)

    def weigh(block, carry):
        pull = []
        for k in range(NVAR):
            pull.append({rc: ratio[window(block, *rc), :] * mass[k, window(block, *rc), :] for rc in tiles})
        for rc in tiles:
            at = window(block, *rc)
            part = [pull[k][rc] * source[k, at, :] for k in range(NVAR)]
            fixed[at, :] = functools.reduce(jnp.add, part)
        for d in range(6):
            for e in range(NVAR):
                line_of = {}
                for rc in tiles:
                    part = blocks[e, 0, 0, d] * pull[0][rc]
                    for k in range(1, NVAR):
                        part = part + blocks[e, k, 0, d] * pull[k][rc]
                    line_of[rc] = part
                if d in (Y_HI, Y_LO, Z_HI, Z_LO):
                    line_of = moved(line_of, {Y_HI: Y_LO, Y_LO: Y_HI, Z_HI: Z_LO, Z_LO: Z_HI}[d])
                for rc in tiles:
                    pulls[d, e, window(block, *rc), :] = line_of[rc]
        return carry

    lax.fori_loop(0, nx, weigh, 0)
    pl.semaphore_wait(gate.at[1], len(line_zl))
    open_gate(2, [mirror])

    def two_parts(value):
        high = value.astype(jnp.bfloat16)
        return high, (value - high.astype(jnp.float32)).astype(jnp.bfloat16)

    def multiply(a, b):
        return jnp.dot(a, b, preferred_element_type=jnp.float32)

    def number_of(shape, dim):
        return lax.broadcasted_iota(jnp.int32, shape, dim)

    def lookup(table, pick, keep):
        spread = jnp.dot(
            table.astype(jnp.float32), pick.astype(jnp.float32), preferred_element_type=jnp.float32
        )
        return jnp.sum(jnp.where(keep, spread, 0.0), axis=0, keepdims=True)

    across, down = number_of((ny, rows), 1), number_of((ny, rows), 0)
    lane, first = number_of((nx, rows), 1), number_of((nx, rows), 0)
    slot_row = lookup(slots[...], lax.rem(across, ny) == down, lax.div(lane, ny) == first)
    each_side(wait_slots)
    beside_row = jnp.where(number_of((1, rows), 1) < 2 * (nx + ny), 0.0, -8.0)
    for side in range(2):
        base_lane = side * ny
        beside_row = beside_row + lookup(
            slots_beside[side],
            across - base_lane == down,
            first == (0 if side else nx - 1),
        )
        base_lane = 2 * ny + side * nx
        beside_row = beside_row + lookup(
            slots_beside[2 + side],
            down == (0 if side else ny - 1),
            lane - base_lane == first,
        )
    n_out = NDES // LANES
    number = number_of((3 * n_out, rows), 0)
    third = lax.div(number, n_out)
    place = lax.rem(number, n_out)
    half_out = n_out // n_core
    row_of = (lax.div(lax.rem(place, half_out), n_x) * n_core + lax.div(place, half_out)) * n_x + lax.rem(place, n_x)
    wanted = 2 * row_of + jnp.where(third == 0, 0, jnp.where(third == 1, -1, 1))
    onehot[:, :rows] = jnp.where(slot_row == wanted.astype(jnp.float32), 1.0, 0.0).astype(jnp.bfloat16)
    onehot[:, rows:] = jnp.where(beside_row == wanted.astype(jnp.float32), 1.0, 0.0).astype(jnp.bfloat16)
    surface[rows:, :] = jnp.zeros_like(surface[rows:, :])
    load_base.wait()
    base_parts[0], base_parts[1] = two_parts(base[...])

    wait_faces(0)
    add_halos(0, relaxed, ratio)
    pack_faces(relaxed, 1)
    send_faces(relaxed, 1)
    def add_surface(block, lo, hi):
        total = {}
        for rc in tiles:
            at = window(block, *rc)
            part = [fixed[at, :]]
            part += [(1.0 - RELAX) * mass[e, at, :] * relaxed[e, at, :] for e in range(NVAR)]
            for d, exists, step in ((X_HI, hi, 1), (X_LO, lo, -1)):
                if exists:
                    part += [pulls[d, e, at, :] * relaxed[e, window(block + step, *rc), :] for e in range(NVAR)]
            total[rc] = functools.reduce(jnp.add, part)
        for d in (Y_HI, Y_LO, Z_HI, Z_LO):
            line_of = {}
            for rc in tiles:
                at = window(block, *rc)
                part = [pulls[d, e, at, :] * relaxed[e, at, :] for e in range(NVAR)]
                line_of[rc] = functools.reduce(jnp.add, part)
            line_of = moved(line_of, d)
            total = {rc: total[rc] + line_of[rc] for rc in tiles}
        for r, c in tiles:
            at = block * ny + r * SUBLANES
            at = at if isinstance(at, int) else pl.multiple_of(at, SUBLANES)
            surface[pl.ds(at, SUBLANES), pl.ds(c * LANES, LANES)] = total[r, c]

    over_blocks(add_surface)
    wait_faces(3)
    for axis, buffer in ((0, halo_x), (1, halo_y)):
        for side in range(2):
            for i, (at, place) in enumerate(face_parts(axis, side)):
                part = [relaxed[e, at, :] * buffer[3, side, e, place, :] for e in range(NVAR)]
                if axis == 0:
                    to = rows + side * ny + (i // n_col) * SUBLANES
                    c = i % n_col
                else:
                    to = rows + 2 * ny + side * nx
                    c = i
                surface[pl.ds(to, SUBLANES), pl.ds(c * LANES, LANES)] = functools.reduce(jnp.add, part)
    high, low = two_parts(surface[...])
    projected = (
        multiply(high, base_parts[1]) + multiply(low, base_parts[0])
    ) + multiply(high, base_parts[0])
    high, low = two_parts(projected)
    looked = multiply(onehot[...], high) + multiply(onehot[...], low)
    even, before, after = (looked[i * n_out : (i + 1) * n_out] for i in range(3))
    half = lax.broadcasted_iota(jnp.int32, (n_out, LANES), 1) < LANES // 2
    swapped = pltpu.roll(jnp.where(half, after, before), LANES // 2, 1)
    whole = jnp.full((n_out, LANES), (weights[0] + weights[1]).astype(jnp.float32))
    mine = jnp.where(cond == 0, weights[0], weights[1]).astype(jnp.float32)
    scaled = (even + swapped) * (jnp.full((n_out, LANES), mine) / whole)

    width = LANES // n_zl
    for q in range(n_zl):
        quarter = scaled if q == 0 else pltpu.roll(scaled, LANES - q * width, 1)
        row_out[pl.ds(q * n_out, n_out)] = quarter[:, :width].reshape(n_out, 1, width)
    pl.semaphore_wait(gate.at[2], 1)

    def piece_copy(target, number):
        return pltpu.make_async_remote_copy(
            src_ref=row_out.at[number],
            dst_ref=column_in.at[device],
            send_sem=column_send,
            recv_sem=column_recv,
            device_id=target,
            device_id_type=MESH,
        )

    for target, number in all_targets:
        piece_copy(target, number).start()
    column_in[device] = row_out[own_piece]
    sweep(relaxed, smoothed)

    wait_faces(1)
    add_halos(1, smoothed, ratio)
    pack_faces(smoothed, 2)
    send_faces(smoothed, 2)
    drain_faces(start, 0)
    drain_faces(None, 3)
    each_side(lambda axis, side: slots_copy(axis, side).wait_send())
    operate(smoothed, residual)
    drain_faces(relaxed, 1)

    wait_faces(2)
    add_halos(2, residual, None)
    drain_faces(smoothed, 2)

    everyone = pltpu.make_async_remote_copy(
        src_ref=column_in.at[pl.ds(0, n_devices - 1)],
        dst_ref=column_in.at[pl.ds(0, n_devices - 1)],
        send_sem=column_send,
        recv_sem=column_recv,
        device_id=(cond, y, core, x, zl),
        device_id_type=MESH,
    )
    everyone.wait_recv()
    groups = 8
    sums = [column_in[i] for i in range(groups)]
    for i in range(groups, n_devices):
        sums[i % groups] = sums[i % groups] + column_in[i]
    row = functools.reduce(jnp.add, sums)
    gradient[...] = row
    everyone.wait_send()


def put_out(*refs):
    count = (len(refs) - 1) // 2
    copies = [pltpu.make_async_copy(refs[i], refs[count + i], refs[-1].at[i]) for i in range(count)]
    for copy in copies:
        copy.start()
    for copy in copies:
        copy.wait()


def to_tiles(array):
    *lead, ny, nz = array.shape
    split = array.reshape(*lead, ny // SUBLANES, SUBLANES, nz // LANES, LANES)
    return jnp.swapaxes(split, -2, -3).reshape(*lead[:-1], -1, LANES)


def from_tiles(array, shape):
    *lead, ny, nz = shape
    split = array.reshape(*lead, ny // SUBLANES, nz // LANES, SUBLANES, LANES)
    return jnp.swapaxes(split, -2, -3).reshape(shape)


def local(
    dims,
    adjoint,
    objective_gradient,
    diagonal,
    flux_blocks,
    flux_sensitivity,
    surface_mask,
    patch_band_slot,
    design_basis,
    condition_weights,
):
    _, nvar, nx, ny, nz = adjoint.shape
    rows = nx * ny
    n_cond, n_y, n_core, n_x, n_zl = dims
    n_plane, n_z = n_y * n_core * n_x, n_cond * n_zl
    f32 = jnp.float32
    flat = nx * ny * nz // LANES
    field, cell = (nvar, flat, LANES), (flat, LANES)
    hbm = pl.BlockSpec(memory_space=pltpu.HBM)
    vmem = pl.BlockSpec(memory_space=pltpu.VMEM)
    dma = pltpu.SemaphoreType.DMA
    smoothed, residual, gradient = pl.pallas_call(
        functools.partial(kernel, dims),
        out_shape=(
            jax.ShapeDtypeStruct(field, f32),
            jax.ShapeDtypeStruct(field, f32),
            jax.ShapeDtypeStruct((1, LANES // n_zl), f32),
        ),
        in_specs=[hbm] * 9,
        out_specs=(vmem, vmem, vmem),
        scratch_shapes=[
            pltpu.SMEM((nvar, nvar, 1, 6), f32),
            pltpu.SMEM((n_cond,), jnp.int32),
            pltpu.VMEM((nx, ny), jnp.int32),
            pltpu.VMEM(field, f32),
            pltpu.VMEM(field, f32),
            pltpu.VMEM(field, f32),
            pltpu.VMEM(cell, f32),
            pltpu.VMEM(cell, f32),
            pltpu.VMEM((nvar, rows, nz), jnp.bfloat16),
            pltpu.VMEM(cell, jnp.int32),
            pltpu.VMEM(design_basis.shape, f32),
            pltpu.VMEM((2 * rows, nz), f32),
            pltpu.VMEM((3 * NDES // LANES, 2 * rows), jnp.bfloat16),
            pltpu.VMEM((2, *design_basis.shape), jnp.bfloat16),
            pltpu.VMEM(field, f32),
            pltpu.VMEM((6, *field), f32),
            pltpu.VMEM(cell, f32),
            pltpu.VMEM((4, 2, nvar, ny * nz // LANES, LANES), f32),
            pltpu.VMEM((4, 2, nvar, nx * nz // LANES, LANES), f32),
            pltpu.VMEM((2, nvar, ny * nz // LANES, LANES), f32),
            pltpu.VMEM((4, 2, nvar, nx * nz // LANES, LANES), f32),
            pltpu.VMEM((4, nx, ny), jnp.int32),
            pltpu.VMEM((n_zl * NDES // LANES, 1, LANES // n_zl), f32),
            pltpu.VMEM((n_cond * n_zl * NDES // LANES, 1, LANES // n_zl), f32),
            dma((9,)),
            dma((4, 4)),
            dma((4, 4)),
            dma((4,)),
            dma((4,)),
            pltpu.SemaphoreType.REGULAR((3,)),
            dma,
            dma,
        ],
        compiler_params=pltpu.CompilerParams(
            collective_id=0, has_side_effects=True, vmem_limit_bytes=KERNEL_VMEM
        ),
        name="adjoint_step",
    )(
        *(
            pltpu.with_memory_space_constraint(a, pltpu.HBM)
            for a in (
                to_tiles(adjoint[0]),
                to_tiles(objective_gradient[0]),
                to_tiles(diagonal),
                flux_sensitivity.reshape(nvar, rows, nz),
                to_tiles(surface_mask),
                design_basis,
                jnp.transpose(flux_blocks, (2, 3, 0, 1)),
                condition_weights,
                patch_band_slot,
            )
        )
    )
    results = (smoothed, residual, gradient)
    smoothed, residual, gradient = pl.pallas_call(
        put_out,
        out_shape=tuple(jax.ShapeDtypeStruct(a.shape, a.dtype) for a in results),
        in_specs=[vmem] * 3,
        out_specs=(hbm,) * 3,
        scratch_shapes=[dma((3,))],
        compiler_params=pltpu.CompilerParams(vmem_limit_bytes=4 * 1024 * 1024),
        name="put_out",
    )(*results)
    whole = (1, nvar, nx, ny, nz)
    return from_tiles(smoothed, whole), from_tiles(residual, whole), gradient.reshape(-1)


def solution(mesh):
    dims = (mesh.shape["cond"], 4, 2, 4, 4)
    torus = Mesh(mesh.devices.reshape(dims), AXES)
    in_specs = (
        P("cond", None, GX, YZ, None),
        P("cond", None, GX, YZ, None),
        P(GX, YZ, None),
        P("cond", None, None, None),
        P("cond", None, GX, YZ, None),
        P(GX, YZ, None),
        P(GX, YZ),
        P(),
        P(),
    )
    out_specs = (P("cond", None, GX, YZ, None), P("cond", None, GX, YZ, None), P(GX_YZ))
    return jax.shard_map(
        functools.partial(local, dims), mesh=torus, in_specs=in_specs, out_specs=out_specs, check_vma=False
    )
```

```python
import functools

import jax
import jax.numpy as jnp
from jax import lax
from jax.experimental import pallas as pl
from jax.experimental.pallas import tpu as pltpu
from jax.sharding import Mesh
from jax.sharding import PartitionSpec as P

NDES = 4096
NVAR = 5
LANES = 128
SUBLANES = 8
AXES = ("cond", "gx_0", "gx_1", "yz_0", "yz_1")
GX = ("gx_0", "gx_1")
YZ = ("yz_0", "yz_1")
GX_YZ = GX + YZ
MESH = pl.DeviceIdType.MESH
RELAX = 0.8
KERNEL_VMEM = 40 * 1024 * 1024
X_HI, X_LO, Y_HI, Y_LO, Z_HI, Z_LO = range(6)


def kernel(
    dims,
    adjoint,
    objective,
    diagonal,
    sensitivity,
    mask,
    basis,
    blocks_in,
    weights_in,
    slots_in,
    smoothed,
    residual,
    gradient,
    blocks,
    weights,
    slots,
    start,
    relaxed,
    source,
    diag,
    ratio,
    sens,
    surface_mask,
    base,
    surface,
    onehot,
    base_parts,
    mass,
    pulls,
    fixed,
    halo_x,
    halo_y,
    face_x,
    face_y,
    slots_beside,
    row_out,
    column_in,
    local_sem,
    halo_send,
    halo_recv,
    slots_send,
    slots_recv,
    gate,
    column_send,
    column_recv,
):
    n_cond, n_y, n_core, n_x, n_zl = dims
    nx, ny = slots.shape
    rows = nx * ny
    n_row, n_col = ny // SUBLANES, basis.shape[0] // LANES
    span = n_row * n_col * SUBLANES
    n_gx, n_yz, n_plane, n_z = n_y * n_core, n_x * n_zl, n_y * n_core * n_x, n_cond * n_zl

    cond, y, core, x, zl = (lax.axis_index(a) for a in AXES)
    gx, yz = y * n_core + core, x * n_zl + zl
    plane, z = gx * n_x + x, cond * n_zl + zl

    def at_gx(g):
        return (cond, lax.div(g, n_core), lax.rem(g, n_core), x, zl)

    def at_yz(q):
        return (cond, y, core, lax.div(q, n_zl), lax.rem(q, n_zl))

    def around(index, size):
        return [index] + [lax.rem(index + o, size) for o in range(1, size)]

    conds, ys, cores, xs, zls = (around(i, n) for i, n in zip((cond, y, core, x, zl), dims))
    steps = [
        (i, j, c, k, l)
        for i in range(n_cond)
        for j in range(n_y)
        for c in range(n_core)
        for k in range(n_x)
        for l in range(n_zl)
        if i or j or c or k or l
    ]
    steps.sort(key=lambda s: -(min(s[1], n_y - s[1]) + min(s[3], n_x - s[3]) + (n_zl if s[0] else s[4])))

    def piece_of(b, c, d, e):
        return ((e * n_core + c) * n_y + b) * n_x + d

    all_targets = [
        ((conds[i], ys[j], cores[c], xs[k], zls[l]), piece_of(ys[j], cores[c], xs[k], zls[l]))
        for i, j, c, k, l in steps
    ]
    n_devices = len(steps) + 1
    own_piece = piece_of(y, core, x, zl)
    device = cond * (n_devices // n_cond) + own_piece

    barrier = pltpu.get_barrier_semaphore()

    def greet(target):
        pl.semaphore_signal(barrier, inc=1, device_id=target, device_id_type=MESH)

    step_up = jnp.logical_and(zl == n_zl - 1, x < n_x - 1)
    step_down = jnp.logical_and(zl == 0, x > 0)

    @pl.when(step_up)
    def _():
        greet(at_yz(yz + 1))

    @pl.when(step_down)
    def _():
        greet(at_yz(yz - 1))

    line_gx = [(cond, b, c, x, zl) for i, b in enumerate(ys) for j, c in enumerate(cores) if i or j]
    mirror = (n_cond - 1 - cond, y, core, x, n_zl - 1 - zl)
    greeted = (
        line_gx + [(cond, y, core, d, zl) for d in xs[1:]] + [(cond, y, core, x, e) for e in zls[1:]] + [mirror]
    )
    for target in greeted:
        greet(target)

    pairs = (
        (adjoint, start),
        (diagonal, diag),
        (objective, source),
        (mask, surface_mask),
        (sensitivity, sens),
        (basis, base),
        (blocks_in, blocks),
        (weights_in, weights),
        (slots_in, slots),
    )
    loads = [pltpu.make_async_copy(a, b, local_sem.at[i]) for i, (a, b) in enumerate(pairs)]
    load_start, load_diag, load_source, load_mask, load_sens, load_base = loads[:6]
    for load in loads:
        load.start()

    sides = (
        (gx > 0, gx < n_gx - 1),
        (yz > 0, yz < n_yz - 1),
    )

    for axis, buffer in ((0, halo_x), (1, halo_y)):
        for side in range(2):

            @pl.when(jnp.logical_not(sides[axis][side]))
            def _(buffer=buffer, side=side, index=2 * axis + side):
                buffer[:, side] = jnp.zeros_like(buffer[:, side])
                slots_beside[index] = jnp.zeros_like(slots_beside[index])

    def halo_copy(field, turn, axis, side):
        index = 2 * axis + side
        if axis == 0:
            if field is None:
                src = face_x.at[side]
            else:
                src = field.at[:, pl.ds((nx - 1) * span if side else 0, span)]
            dst = halo_x.at[turn, 1 - side]
            target = at_gx(gx + 1 if side else gx - 1)
        else:
            src = face_y.at[turn, side]
            dst = halo_y.at[turn, 1 - side]
            target = at_yz(yz + 1 if side else yz - 1)
        return pltpu.make_async_remote_copy(
            src_ref=src,
            dst_ref=dst,
            send_sem=halo_send.at[turn, index],
            recv_sem=halo_recv.at[turn, 2 * axis + 1 - side],
            device_id=target,
            device_id_type=MESH,
        )

    def each_side(body):
        for axis in (1, 0):
            for side in range(2):

                @pl.when(sides[axis][side])
                def _(axis=axis, side=side):
                    body(axis, side)

    def line(side, c):
        first = ((n_row - 1) * n_col + c) * SUBLANES + SUBLANES - 1 if side else c * SUBLANES
        return pl.ds(first, nx, stride=span)

    def pack_faces(field, turn):
        for side in range(2):
            for e in range(NVAR):
                for c in range(n_col):
                    face_y[turn, side, e, pl.ds(c * nx, nx), :] = field[e, line(side, c), :]

    far = (zl == 0, zl == n_zl - 1)

    def send_far(field, turn):
        for side in range(2):

            @pl.when(jnp.logical_and(sides[1][side], far[side]))
            def _(side=side):
                halo_copy(field, turn, 1, side).start()

    def send_near(field, turn):
        for side in range(2):

            @pl.when(jnp.logical_not(far[side]))
            def _(side=side):
                halo_copy(field, turn, 1, side).start()

        for side in range(2):

            @pl.when(sides[0][side])
            def _(side=side):
                halo_copy(field, turn, 0, side).start()

    def send_faces(field, turn):
        send_far(field, turn)
        send_near(field, turn)

    def slots_copy(axis, side):
        index = 2 * axis + side
        if axis == 0:
            target = at_gx(gx + 1 if side else gx - 1)
        else:
            target = at_yz(yz + 1 if side else yz - 1)
        return pltpu.make_async_remote_copy(
            src_ref=slots,
            dst_ref=slots_beside.at[2 * axis + 1 - side],
            send_sem=slots_send.at[index],
            recv_sem=slots_recv.at[2 * axis + 1 - side],
            device_id=target,
            device_id_type=MESH,
        )

    def wait_slots(axis, side):
        index = 2 * axis + side
        pltpu.make_async_remote_copy(
            src_ref=slots,
            dst_ref=slots_beside.at[index],
            send_sem=slots_send.at[index],
            recv_sem=slots_recv.at[index],
            device_id=(cond, y, core, x, zl),
            device_id_type=MESH,
        ).wait_recv()

    def wait_faces(turn):
        def body(axis, side):
            pltpu.make_async_remote_copy(
                src_ref=(halo_x if axis == 0 else halo_y).at[turn, side],
                dst_ref=(halo_x if axis == 0 else halo_y).at[turn, side],
                send_sem=halo_send.at[turn, 2 * axis + side],
                recv_sem=halo_recv.at[turn, 2 * axis + side],
                device_id=(cond, y, core, x, zl),
                device_id_type=MESH,
            ).wait_recv()

        each_side(body)

    def drain_faces(field, turn):
        each_side(lambda axis, side: halo_copy(field, turn, axis, side).wait_send())

    tiles = [(r, c) for r in range(n_row) for c in range(n_col)]

    def window(block, r, c):
        at = block * span + (r * n_col + c) * SUBLANES
        return pl.ds(at if isinstance(at, int) else pl.multiple_of(at, SUBLANES), SUBLANES)

    def moved(here, d):
        axis, size, up = (0 if d in (Y_HI, Y_LO) else 1), (SUBLANES if d in (Y_HI, Y_LO) else LANES), d in (Y_HI, Z_HI)
        index = lax.broadcasted_iota(jnp.int32, (SUBLANES, LANES), axis)
        zero = jnp.zeros((SUBLANES, LANES), jnp.float32)
        edge, shift, step = (size - 1, size - 1, 1) if up else (0, 1, -1)
        turned = {rc: pltpu.roll(here[rc], shift, axis) for rc in tiles}
        return {
            (r, c): jnp.where(
                index == edge, turned.get((r + step, c) if axis == 0 else (r, c + step), zero), turned[r, c]
            )
            for r, c in tiles
        }

    def neighbours(field, block, lo, hi):
        def tile_of(e, b, r, c):
            return field[e, window(b, r, c), :]

        total = [[None] * len(tiles) for _ in range(NVAR)]
        for e in range(NVAR):
            here = {rc: tile_of(e, block, *rc) for rc in tiles}
            terms = {}
            if hi:
                terms[X_HI] = {rc: tile_of(e, block + 1, *rc) for rc in tiles}
            if lo:
                terms[X_LO] = {rc: tile_of(e, block - 1, *rc) for rc in tiles}
            for d in (Y_HI, Y_LO, Z_HI, Z_LO):
                terms[d] = moved(here, d)
            for d, values in terms.items():
                for k in range(NVAR):
                    coef = blocks[e, k, 0, d]
                    for i, rc in enumerate(tiles):
                        part = coef * values[rc]
                        total[k][i] = part if total[k][i] is None else total[k][i] + part
        return total

    def over_blocks(body, between=None):
        body(0, False, True)

        def inner(b, carry):
            body(b, True, True)
            return carry

        if between is None:
            lax.fori_loop(1, nx - 1, inner, 0)
        else:
            lax.fori_loop(1, nx - 2, inner, 0)
            between()
            lax.fori_loop(nx - 2, nx - 1, inner, 0)
        body(nx - 1, True, False)

    def sweep(field, result, between=None):
        def body(block, lo, hi):
            total = neighbours(field, block, lo, hi)
            for i, rc in enumerate(tiles):
                at = window(block, *rc)
                scale = ratio[at, :]
                for k in range(NVAR):
                    result[k, at, :] = (1.0 - RELAX) * field[k, at, :] + scale * (
                        source[k, at, :] + total[k][i]
                    )

        over_blocks(body, between)

    def operate(field, result):
        def body(block, lo, hi):
            total = neighbours(field, block, lo, hi)
            for i, rc in enumerate(tiles):
                at = window(block, *rc)
                scale = diag[at, :]
                for k in range(NVAR):
                    result[k, at, :] = source[k, at, :] - scale * field[k, at, :] + total[k][i]

        over_blocks(body)

    def face_parts(axis, side):
        if axis == 0:
            first = (nx - 1) * span if side else 0
            return [(pl.ds(first + i, SUBLANES), pl.ds(i, SUBLANES)) for i in range(0, span, SUBLANES)]
        return [(line(side, c), pl.ds(c * nx, nx)) for c in range(n_col)]

    def add_halos(turn, result, scale):
        for axis, buffer in ((0, halo_x), (1, halo_y)):
            for side in range(2):
                d = (X_LO, X_HI, Y_LO, Y_HI)[2 * axis + side]
                for at, place in face_parts(axis, side):
                    factor = None if scale is None else scale[at, :]
                    outside = [buffer[turn, side, e, place, :] for e in range(NVAR)]
                    for k in range(NVAR):
                        part = blocks[0, k, 0, d] * outside[0]
                        for e in range(1, NVAR):
                            part = part + blocks[e, k, 0, d] * outside[e]
                        part = part if factor is None else factor * part
                        result[k, at, :] = result[k, at, :] + part

    load_start.wait()
    pack_faces(start, 0)
    for load in loads[6:]:
        load.wait()
    load_diag.wait()
    ratio[...] = RELAX / diag[...]
    load_mask.wait()
    load_sens.wait()
    for block in range(nx):
        for c in range(n_col):
            cols = pl.ds(c * LANES, LANES)
            for k in range(NVAR):
                weight = sens[k, pl.ds(block * ny, ny), cols].astype(jnp.float32)
                for r in range(n_row):
                    at = window(block, r, c)
                    mass[k, at, :] = (
                        surface_mask[at, :].astype(jnp.float32) * weight[r * SUBLANES : (r + 1) * SUBLANES]
                    )
    for axis, faces in ((1, face_y.at[3]), (0, face_x)):
        for side in range(2):
            d = (X_LO, X_HI, Y_LO, Y_HI)[2 * axis + side]
            for at, place in face_parts(axis, side):
                pull = [ratio[at, :] * mass[k, at, :] for k in range(NVAR)]
                for e in range(NVAR):
                    part = blocks[e, 0, 0, d] * pull[0]
                    for k in range(1, NVAR):
                        part = part + blocks[e, k, 0, d] * pull[k]
                    faces[side, e, place, :] = part
    pl.semaphore_wait(
        barrier, len(greeted) + step_up.astype(jnp.int32) + step_down.astype(jnp.int32)
    )
    send_far(start, 0)
    each_side(lambda axis, side: slots_copy(axis, side).start())
    line_zl = [(cond, y, core, x, e) for e in zls[1:]]

    def open_gate(i, targets):
        for target in targets:
            pl.semaphore_signal(gate.at[i], inc=1, device_id=target, device_id_type=MESH)

    open_gate(0, line_gx)


    load_source.wait()

    def second_gate():
        send_far(None, 3)
        send_near(None, 3)
        pl.semaphore_wait(gate.at[0], len(line_gx))
        open_gate(1, line_zl)

    send_near(start, 0)
    sweep(start, relaxed, second_gate)

    def weigh(block, carry):
        pull = []
        for k in range(NVAR):
            pull.append({rc: ratio[window(block, *rc), :] * mass[k, window(block, *rc), :] for rc in tiles})
        for rc in tiles:
            at = window(block, *rc)
            part = [pull[k][rc] * source[k, at, :] for k in range(NVAR)]
            fixed[at, :] = functools.reduce(jnp.add, part)
        for d in range(6):
            for e in range(NVAR):
                line_of = {}
                for rc in tiles:
                    part = blocks[e, 0, 0, d] * pull[0][rc]
                    for k in range(1, NVAR):
                        part = part + blocks[e, k, 0, d] * pull[k][rc]
                    line_of[rc] = part
                if d in (Y_HI, Y_LO, Z_HI, Z_LO):
                    line_of = moved(line_of, {Y_HI: Y_LO, Y_LO: Y_HI, Z_HI: Z_LO, Z_LO: Z_HI}[d])
                for rc in tiles:
                    pulls[d, e, window(block, *rc), :] = line_of[rc]
        return carry

    lax.fori_loop(0, nx, weigh, 0)
    pl.semaphore_wait(gate.at[1], len(line_zl))
    open_gate(2, [mirror])

    def two_parts(value):
        high = value.astype(jnp.bfloat16)
        return high, (value - high.astype(jnp.float32)).astype(jnp.bfloat16)

    def multiply(a, b):
        return jnp.dot(a, b, preferred_element_type=jnp.float32)

    def number_of(shape, dim):
        return lax.broadcasted_iota(jnp.int32, shape, dim)

    def lookup(table, pick, keep):
        spread = jnp.dot(
            table.astype(jnp.float32), pick.astype(jnp.float32), preferred_element_type=jnp.float32
        )
        return jnp.sum(jnp.where(keep, spread, 0.0), axis=0, keepdims=True)

    across, down = number_of((ny, rows), 1), number_of((ny, rows), 0)
    lane, first = number_of((nx, rows), 1), number_of((nx, rows), 0)
    slot_row = lookup(slots[...], lax.rem(across, ny) == down, lax.div(lane, ny) == first)
    each_side(wait_slots)
    beside_row = jnp.where(number_of((1, rows), 1) < 2 * (nx + ny), 0.0, -8.0)
    for side in range(2):
        base_lane = side * ny
        beside_row = beside_row + lookup(
            slots_beside[side],
            across - base_lane == down,
            first == (0 if side else nx - 1),
        )
        base_lane = 2 * ny + side * nx
        beside_row = beside_row + lookup(
            slots_beside[2 + side],
            down == (0 if side else ny - 1),
            lane - base_lane == first,
        )
    n_out = NDES // LANES
    number = number_of((3 * n_out, rows), 0)
    third = lax.div(number, n_out)
    place = lax.rem(number, n_out)
    half_out = n_out // n_core
    row_of = (lax.div(lax.rem(place, half_out), n_x) * n_core + lax.div(place, half_out)) * n_x + lax.rem(place, n_x)
    wanted = 2 * row_of + jnp.where(third == 0, 0, jnp.where(third == 1, -1, 1))
    onehot[:, :rows] = jnp.where(slot_row == wanted.astype(jnp.float32), 1.0, 0.0).astype(jnp.bfloat16)
    onehot[:, rows:] = jnp.where(beside_row == wanted.astype(jnp.float32), 1.0, 0.0).astype(jnp.bfloat16)
    surface[rows:, :] = jnp.zeros_like(surface[rows:, :])
    load_base.wait()
    base_parts[0], base_parts[1] = two_parts(base[...])

    wait_faces(0)
    add_halos(0, relaxed, ratio)
    pack_faces(relaxed, 1)
    send_faces(relaxed, 1)
    def add_surface(block, lo, hi):
        total = {}
        for rc in tiles:
            at = window(block, *rc)
            part = [fixed[at, :]]
            part += [(1.0 - RELAX) * mass[e, at, :] * relaxed[e, at, :] for e in range(NVAR)]
            for d, exists, step in ((X_HI, hi, 1), (X_LO, lo, -1)):
                if exists:
                    part += [pulls[d, e, at, :] * relaxed[e, window(block + step, *rc), :] for e in range(NVAR)]
            total[rc] = functools.reduce(jnp.add, part)
        for d in (Y_HI, Y_LO, Z_HI, Z_LO):
            line_of = {}
            for rc in tiles:
                at = window(block, *rc)
                part = [pulls[d, e, at, :] * relaxed[e, at, :] for e in range(NVAR)]
                line_of[rc] = functools.reduce(jnp.add, part)
            line_of = moved(line_of, d)
            total = {rc: total[rc] + line_of[rc] for rc in tiles}
        for r, c in tiles:
            at = block * ny + r * SUBLANES
            at = at if isinstance(at, int) else pl.multiple_of(at, SUBLANES)
            surface[pl.ds(at, SUBLANES), pl.ds(c * LANES, LANES)] = total[r, c]

    over_blocks(add_surface)
    wait_faces(3)
    for axis, buffer in ((0, halo_x), (1, halo_y)):
        for side in range(2):
            for i, (at, place) in enumerate(face_parts(axis, side)):
                part = [relaxed[e, at, :] * buffer[3, side, e, place, :] for e in range(NVAR)]
                if axis == 0:
                    to = rows + side * ny + (i // n_col) * SUBLANES
                    c = i % n_col
                else:
                    to = rows + 2 * ny + side * nx
                    c = i
                surface[pl.ds(to, SUBLANES), pl.ds(c * LANES, LANES)] = functools.reduce(jnp.add, part)
    high, low = two_parts(surface[...])
    projected = (
        multiply(high, base_parts[1]) + multiply(low, base_parts[0])
    ) + multiply(high, base_parts[0])
    high, low = two_parts(projected)
    looked = multiply(onehot[...], high) + multiply(onehot[...], low)
    even, before, after = (looked[i * n_out : (i + 1) * n_out] for i in range(3))
    half = lax.broadcasted_iota(jnp.int32, (n_out, LANES), 1) < LANES // 2
    swapped = pltpu.roll(jnp.where(half, after, before), LANES // 2, 1)
    whole = jnp.full((n_out, LANES), (weights[0] + weights[1]).astype(jnp.float32))
    mine = jnp.where(cond == 0, weights[0], weights[1]).astype(jnp.float32)
    scaled = (even + swapped) * (jnp.full((n_out, LANES), mine) / whole)

    width = LANES // n_zl
    for q in range(n_zl):
        quarter = scaled if q == 0 else pltpu.roll(scaled, LANES - q * width, 1)
        row_out[pl.ds(q * n_out, n_out)] = quarter[:, :width].reshape(n_out, 1, width)
    pl.semaphore_wait(gate.at[2], 1)

    def piece_copy(target, number):
        return pltpu.make_async_remote_copy(
            src_ref=row_out.at[number],
            dst_ref=column_in.at[device],
            send_sem=column_send,
            recv_sem=column_recv,
            device_id=target,
            device_id_type=MESH,
        )

    for target, number in all_targets:
        piece_copy(target, number).start()
    column_in[device] = row_out[own_piece]
    sweep(relaxed, smoothed)

    wait_faces(1)
    add_halos(1, smoothed, ratio)
    pack_faces(smoothed, 2)
    send_faces(smoothed, 2)
    drain_faces(start, 0)
    drain_faces(None, 3)
    each_side(lambda axis, side: slots_copy(axis, side).wait_send())
    operate(smoothed, residual)
    drain_faces(relaxed, 1)

    wait_faces(2)
    add_halos(2, residual, None)
    drain_faces(smoothed, 2)

    everyone = pltpu.make_async_remote_copy(
        src_ref=column_in.at[pl.ds(0, n_devices - 1)],
        dst_ref=column_in.at[pl.ds(0, n_devices - 1)],
        send_sem=column_send,
        recv_sem=column_recv,
        device_id=(cond, y, core, x, zl),
        device_id_type=MESH,
    )
    everyone.wait_recv()
    row = jnp.sum(column_in[...].reshape(n_devices, LANES // n_zl), axis=0, keepdims=True)
    gradient[...] = row
    everyone.wait_send()


def put_out(*refs):
    count = (len(refs) - 1) // 2
    copies = [pltpu.make_async_copy(refs[i], refs[count + i], refs[-1].at[i]) for i in range(count)]
    for copy in copies:
        copy.start()
    for copy in copies:
        copy.wait()


def to_tiles(array):
    *lead, ny, nz = array.shape
    split = array.reshape(*lead, ny // SUBLANES, SUBLANES, nz // LANES, LANES)
    return jnp.swapaxes(split, -2, -3).reshape(*lead[:-1], -1, LANES)


def from_tiles(array, shape):
    *lead, ny, nz = shape
    split = array.reshape(*lead, ny // SUBLANES, nz // LANES, SUBLANES, LANES)
    return jnp.swapaxes(split, -2, -3).reshape(shape)


def local(
    dims,
    adjoint,
    objective_gradient,
    diagonal,
    flux_blocks,
    flux_sensitivity,
    surface_mask,
    patch_band_slot,
    design_basis,
    condition_weights,
):
    _, nvar, nx, ny, nz = adjoint.shape
    rows = nx * ny
    n_cond, n_y, n_core, n_x, n_zl = dims
    n_plane, n_z = n_y * n_core * n_x, n_cond * n_zl
    f32 = jnp.float32
    flat = nx * ny * nz // LANES
    field, cell = (nvar, flat, LANES), (flat, LANES)
    hbm = pl.BlockSpec(memory_space=pltpu.HBM)
    vmem = pl.BlockSpec(memory_space=pltpu.VMEM)
    dma = pltpu.SemaphoreType.DMA
    smoothed, residual, gradient = pl.pallas_call(
        functools.partial(kernel, dims),
        out_shape=(
            jax.ShapeDtypeStruct(field, f32),
            jax.ShapeDtypeStruct(field, f32),
            jax.ShapeDtypeStruct((1, LANES // n_zl), f32),
        ),
        in_specs=[hbm] * 9,
        out_specs=(vmem, vmem, vmem),
        scratch_shapes=[
            pltpu.SMEM((nvar, nvar, 1, 6), f32),
            pltpu.SMEM((n_cond,), jnp.int32),
            pltpu.VMEM((nx, ny), jnp.int32),
            pltpu.VMEM(field, f32),
            pltpu.VMEM(field, f32),
            pltpu.VMEM(field, f32),
            pltpu.VMEM(cell, f32),
            pltpu.VMEM(cell, f32),
            pltpu.VMEM((nvar, rows, nz), jnp.bfloat16),
            pltpu.VMEM(cell, jnp.int32),
            pltpu.VMEM(design_basis.shape, f32),
            pltpu.VMEM((2 * rows, nz), f32),
            pltpu.VMEM((3 * NDES // LANES, 2 * rows), jnp.bfloat16),
            pltpu.VMEM((2, *design_basis.shape), jnp.bfloat16),
            pltpu.VMEM(field, f32),
            pltpu.VMEM((6, *field), f32),
            pltpu.VMEM(cell, f32),
            pltpu.VMEM((4, 2, nvar, ny * nz // LANES, LANES), f32),
            pltpu.VMEM((4, 2, nvar, nx * nz // LANES, LANES), f32),
            pltpu.VMEM((2, nvar, ny * nz // LANES, LANES), f32),
            pltpu.VMEM((4, 2, nvar, nx * nz // LANES, LANES), f32),
            pltpu.VMEM((4, nx, ny), jnp.int32),
            pltpu.VMEM((n_zl * NDES // LANES, 1, LANES // n_zl), f32),
            pltpu.VMEM((n_cond * n_zl * NDES // LANES, 1, LANES // n_zl), f32),
            dma((9,)),
            dma((4, 4)),
            dma((4, 4)),
            dma((4,)),
            dma((4,)),
            pltpu.SemaphoreType.REGULAR((3,)),
            dma,
            dma,
        ],
        compiler_params=pltpu.CompilerParams(
            collective_id=0, has_side_effects=True, vmem_limit_bytes=KERNEL_VMEM
        ),
        name="adjoint_step",
    )(
        *(
            pltpu.with_memory_space_constraint(a, pltpu.HBM)
            for a in (
                to_tiles(adjoint[0]),
                to_tiles(objective_gradient[0]),
                to_tiles(diagonal),
                flux_sensitivity.reshape(nvar, rows, nz),
                to_tiles(surface_mask),
                design_basis,
                jnp.transpose(flux_blocks, (2, 3, 0, 1)),
                condition_weights,
                patch_band_slot,
            )
        )
    )
    results = (smoothed, residual, gradient)
    smoothed, residual, gradient = pl.pallas_call(
        put_out,
        out_shape=tuple(jax.ShapeDtypeStruct(a.shape, a.dtype) for a in results),
        in_specs=[vmem] * 3,
        out_specs=(hbm,) * 3,
        scratch_shapes=[dma((3,))],
        compiler_params=pltpu.CompilerParams(vmem_limit_bytes=4 * 1024 * 1024),
        name="put_out",
    )(*results)
    whole = (1, nvar, nx, ny, nz)
    return from_tiles(smoothed, whole), from_tiles(residual, whole), gradient.reshape(-1)


def solution(mesh):
    dims = (mesh.shape["cond"], 4, 2, 4, 4)
    torus = Mesh(mesh.devices.reshape(dims), AXES)
    in_specs = (
        P("cond", None, GX, YZ, None),
        P("cond", None, GX, YZ, None),
        P(GX, YZ, None),
        P("cond", None, None, None),
        P("cond", None, GX, YZ, None),
        P(GX, YZ, None),
        P(GX, YZ),
        P(),
        P(),
    )
    out_specs = (P("cond", None, GX, YZ, None), P("cond", None, GX, YZ, None), P(GX_YZ))
    return jax.shard_map(
        functools.partial(local, dims), mesh=torus, in_specs=in_specs, out_specs=out_specs, check_vma=False
    )
```
